128 devices in a mesh: blk: 16 (over z_lo, y, core), seq: 8 (over x, z_hi).
Axes of the slice: x: 4, y: 4, z: 4 (z_hi: 2, z_lo: 2; z = z_hi * 2 + z_lo), core: 2. Of those that a mesh axis runs over, the one named last changes fastest.
Arguments:
- layer_input: bfloat16 [16, 1024, 8192], P('blk', 'seq'), may hold values from -6 to 6
- queries: bfloat16 [16, 1024, 4096], P('blk', 'seq'), may hold values from -48 to 48, as said below
- grad_out: bfloat16 [16, 1024, 4096], P('blk', 'seq'), may hold values from -6 to 6
- segment_ids: int32 [16, 1024], P('blk', 'seq'), may hold values from 0 to 3, never falling along the last dimension, each value on 1 to 512 neighbouring positions
- kv_weight: bfloat16 [8192, 1024], P(('blk', 'seq')), may hold values from -0.0625 to 0.0625
- norm_gain: float32 [8192], replicated, may hold values from 0.5 to 1.5
Outputs:
- attended: bfloat16 [16, 1024, 4096], P('blk', 'seq')
- grad_queries: bfloat16 [16, 1024, 4096], P('blk', 'seq')
- grad_input: bfloat16 [16, 1024, 8192], P('blk', 'seq')
- grad_weight: float32 [8192, 1024], P(('blk', 'seq'))
- grad_gain: float32 [8192], replicated
The draws below stay inside these ranges and needn't reach their ends.
Inputs may be any that keep to these rules, and one draw needn't show every extreme that they name: Projected queries; some rows may be larger than others.
All inputs are finite; a program needn't handle non-finite values.
Results may differ from the reference program's by a relative error of at most 0.02.
The reference program's roundings to bfloat16 on the way count: a program that leaves them out, or rounds other values in their place, can miss the bound.
Values may be sent and summed in bfloat16 or wider, within the bound.
No kernel may reach another device: no remote copies, remote signals or barrier semaphores. Data moves between devices by JAX's collectives and lax.ppermute only.
A program may use at most 128 MiB of HBM per device.

```python
import math
import jax
import jax.numpy as jnp
import numpy as np
from jax import lax

D = 8192
HEAD = 128
KV_HEADS = 4
Q_HEADS = 32
LENGTH = 1024
QW = 4096
KVC = 1024
N_BLK = 16


def draw_queries(key, part):
    base = jax.random.normal(key, (N_BLK, LENGTH, QW), jnp.float32)
    base = jnp.clip(base, -4.0, 4.0)
    return base.astype(jnp.bfloat16)


def block_levels(rng, dims, cuts, smallest, top_value):
    def one(axis_at, shards_of):
        heights = jax.random.uniform(jax.random.fold_in(jax.random.fold_in(rng, 6), axis_at), (shards_of,), jnp.float32, smallest / len(cuts), top_value / len(cuts))
        return jnp.repeat(jnp.exp(heights), dims[axis_at] // shards_of).reshape((-1,) + (1,) * (len(dims) - axis_at - 1))

    level = one(*cuts[0])
    for cut in cuts[1:]:
        level = level * one(*cut)
    return level


def length_profile(amount, total, bound, slope):
    loads = [(1 << 20) // math.isqrt(standing ** slope) + 1 for standing in range(2, amount + 1)]
    surplus, given = total - bound - (amount - 1), [1] * (amount - 1)
    while surplus > 0:
        movable = [i for i in range(amount - 1) if given[i] < bound]
        whole, budget = sum([loads[i] for i in movable]), surplus
        for i in movable:
            more = min(bound - given[i], max(1, budget * loads[i] // whole), surplus)
            given[i] = given[i] + more
            surplus = surplus - more
    return np.array([bound] + given)


def uneven_parts(rng, amount, total, limit, lean):
    if amount == 2:
        one = jax.random.randint(rng, (), max(1, total - limit), min(limit, total - 1) + 1)
        return jnp.stack([one, total - one])
    sizes = jnp.asarray(length_profile(amount, total, limit, lean), jnp.int32)
    pairs = (amount - 1) // 2
    donor, taker = sizes[1:1 + 2 * pairs:2], sizes[2:2 + 2 * pairs:2]
    slack = jnp.minimum(donor - 1, limit - taker)
    passed = jax.random.randint(jax.random.fold_in(rng, 1), (pairs,), 0, 1 << 20) % (slack + 1)
    sizes = sizes.at[1:1 + 2 * pairs:2].set(donor - passed).at[2:2 + 2 * pairs:2].set(taker + passed)
    return sizes[jax.random.permutation(jax.random.fold_in(rng, 2), amount)]


def bell_draw(stream_key, dims, width, most, shards=(), dtype=jnp.bfloat16):
    drawn = width * jax.random.normal(stream_key, dims, jnp.float32)
    if shards:
        drawn = drawn * block_levels(stream_key, dims, shards, -0.22, 0.18)
    return jnp.clip(drawn, -most, most).astype(dtype)


def setup_inputs(seed: int = 0) -> dict:
    keys = jax.random.split(jax.random.key(seed), 7)
    return {
        "layer_input": bell_draw(keys[0], (N_BLK, LENGTH, D), 1.0, 6.0, ((0, 16), (1, 8))),
        "queries": draw_queries(jax.random.fold_in(keys[6], 71), 0),
        "grad_out": bell_draw(keys[2], (N_BLK, LENGTH, QW), 1.0, 6.0, ((0, 16), (1, 8))),
        "segment_ids": jax.vmap(lambda own: jnp.searchsorted(jnp.cumsum(uneven_parts(own, 4, LENGTH, LENGTH // 2, 2)), jnp.arange(LENGTH), side="right"))(jax.random.split(keys[3], N_BLK)).reshape((N_BLK, LENGTH)).astype(jnp.int32),
        "kv_weight": bell_draw(keys[4], (D, KVC), D ** -0.5, 0.0625, ((0, 128),)),
        "norm_gain": jnp.clip(1.0 + 0.1 * jax.random.normal(keys[5], (D,), jnp.float32), 0.5, 1.5),
    }


epsilon = 1e-05

def per_sequence(layer_row, query_row, grad_row, segment_row, kv_weight, norm_gain):
    f32 = jnp.float32
    kv_width = KV_HEADS * HEAD
    group_size = Q_HEADS // KV_HEADS
    score_scale = HEAD ** (-0.5)
    source = layer_row.astype(f32)
    inv_rms = lax.rsqrt(lax.optimization_barrier(jnp.mean(source * source, axis=1, keepdims=True)) + epsilon)
    scaled = source * inv_rms
    normed = (scaled * norm_gain).astype(jnp.bfloat16)
    kv_rows = jnp.dot(normed, kv_weight, preferred_element_type=f32).astype(jnp.bfloat16)
    key_heads = kv_rows[:, :kv_width].reshape(LENGTH, KV_HEADS, HEAD).astype(f32)
    value_heads = kv_rows[:, kv_width:].reshape(LENGTH, KV_HEADS, HEAD).astype(f32)
    query_heads = query_row.reshape(LENGTH, KV_HEADS, group_size, HEAD).astype(f32)
    raw_scores = jnp.einsum('qgjd,kgd->gjqk', query_heads, key_heads) * score_scale
    positions = jnp.arange(LENGTH)
    allowed = (positions[None, :] <= positions[:, None]) & (segment_row[None, :] == segment_row[:, None])
    masked = jnp.where(allowed, raw_scores, -1e+30)
    row_max = lax.optimization_barrier(jnp.max(masked, axis=-1, keepdims=True))
    expo_terms = jnp.where(allowed, jnp.exp(masked - row_max), 0.0)
    row_sum = lax.optimization_barrier(jnp.sum(expo_terms, axis=-1, keepdims=True))
    weights = expo_terms.astype(jnp.bfloat16).astype(f32)
    summed = jnp.einsum('gjqk,kgd->gjqd', weights, value_heads) / row_sum
    attended = summed.transpose(2, 0, 1, 3).reshape(LENGTH, QW).astype(jnp.bfloat16)
    log_total = row_max + jnp.log(row_sum)
    softmax_probs = jnp.where(allowed, jnp.exp(masked - log_total), 0.0)
    grad_heads = grad_row.reshape(LENGTH, KV_HEADS, group_size, HEAD).astype(f32).transpose(1, 2, 0, 3)
    attended_heads = attended.reshape(LENGTH, KV_HEADS, group_size, HEAD).astype(f32).transpose(1, 2, 0, 3)
    row_delta = lax.optimization_barrier(jnp.sum(grad_heads * attended_heads, axis=-1, keepdims=True))
    grad_probs = jnp.einsum('gjqd,kgd->gjqk', grad_heads, value_heads)
    grad_scores = (softmax_probs * (grad_probs - row_delta)).astype(jnp.bfloat16).astype(f32)
    probs_half = softmax_probs.astype(jnp.bfloat16).astype(f32)
    grad_values = jnp.einsum('gjqk,gjqd->kgd', probs_half, grad_heads)
    grad_keys = jnp.einsum('gjqk,qgjd->kgd', grad_scores, query_heads) * score_scale
    grad_query = jnp.einsum('gjqk,kgd->qgjd', grad_scores, key_heads) * score_scale
    grad_query = grad_query.reshape(LENGTH, QW).astype(jnp.bfloat16)
    grad_kv = jnp.concatenate([grad_keys.reshape(LENGTH, kv_width), grad_values.reshape(LENGTH, kv_width)], axis=1).astype(jnp.bfloat16)
    weight_term = lax.dot_general(normed, grad_kv, (((0,), (0,)), ((), ())), preferred_element_type=f32)
    grad_normed = lax.dot_general(grad_kv, kv_weight, (((1,), (1,)), ((), ())), preferred_element_type=f32).astype(jnp.bfloat16)
    grad_norm = grad_normed.astype(f32)
    gain_term = lax.optimization_barrier(jnp.sum(grad_norm * scaled, axis=0))
    grad_hat = grad_norm * norm_gain
    grad_input = inv_rms * (grad_hat - scaled * lax.optimization_barrier(jnp.mean(grad_hat * scaled, axis=1, keepdims=True)))
    return (attended, grad_query, grad_input.astype(jnp.bfloat16), weight_term, gain_term)

def reference(layer_input, queries, grad_out, segment_ids, kv_weight, norm_gain):

    def apply_one(bundle):
        return per_sequence(bundle[0], bundle[1], bundle[2], bundle[3], kv_weight, norm_gain)
    attended, grad_queries, grad_input, weight_terms, gain_terms = lax.map(apply_one, (layer_input, queries, grad_out, segment_ids))
    return (attended, grad_queries, grad_input, lax.optimization_barrier(jnp.sum(weight_terms, axis=0)), lax.optimization_barrier(jnp.sum(gain_terms, axis=0)))
```

```python
import jax
import jax.numpy as jnp
from jax import lax
from jax.experimental import pallas as pl
from jax.experimental.pallas import tpu as pltpu
from jax.sharding import Mesh, PartitionSpec as P

HEAD = 128
UNIT = 128
BACK = 4
EPSILON = 1e-05
BF16 = jnp.bfloat16
F32 = jnp.float32
VMEM_LIMIT = 56 * 1024 * 1024

SIZES = {"zlo": 2, "y": 4, "core": 2, "x": 4, "zhi": 2}
BLK = ("zlo", "y", "core")
SEQ = ("x", "zhi")
REL4 = (0, -1, 1, 2)


def shift(value, axis, by):
    n = SIZES[axis]
    return lax.ppermute(value, axis, [(i, (i + by) % n) for i in range(n)])


def shift_seq(value, by):
    n = SIZES["x"] * SIZES["zhi"]
    pairs = [(i, i + by) for i in range(n) if 0 <= i + by < n]
    return lax.ppermute(value, SEQ, pairs)


def rows(pieces):
    return jnp.concatenate(pieces, axis=0)


def ring4(value, axis):
    half = value.shape[0] // 2
    before = shift(value, axis, 1)
    after = shift(value, axis, -1)
    return [value, before, after, shift(before[:half], axis, 1), shift(after[half:], axis, -1)]


def gather_weight(weight):
    other = shift(weight, "zhi", 1)
    unit = jnp.where(
        lax.axis_index("zhi") == 0, rows([weight, other]), rows([other, weight])
    )
    half = unit.shape[1] // 2
    pair = rows([unit, shift(unit, "zlo", 1)])
    left = rows(ring4(pair[:, :half], "y"))
    right = rows(ring4(pair[:, half:], "x"))
    return ring4(left, "x"), ring4(right, "y")


def unit_table():
    zlo, y, x = lax.axis_index("zlo"), lax.axis_index("y"), lax.axis_index("x")
    rel = jnp.array(REL4, jnp.int32)
    zs = (zlo + jnp.arange(2, dtype=jnp.int32)) % 2
    ys, xs = (y + rel) % 4, (x + rel) % 4
    left = (zs[None, None, :] * 4 + ys[None, :, None]) * 4 + xs[:, None, None]
    right = (zs[None, None, :] * 4 + ys[:, None, None]) * 4 + xs[None, :, None]
    return jnp.stack([left, right]).reshape(64).astype(jnp.int32)


PIECES = tuple(
    (side, side * 32 + first, count)
    for side in (0, 1)
    for first, count in ((0, 8), (8, 8), (16, 8), (24, 4), (28, 4))
)


def norm_kernel(core_ref, x_ref, gain_ref, own_ref, send_ref, inv_ref):
    source = x_ref[...].astype(F32)
    inv = lax.rsqrt(jnp.mean(source * source, axis=1, keepdims=True) + EPSILON)
    inv_ref[...] = jnp.broadcast_to(inv, inv_ref.shape)
    first = core_ref[0] == 0
    for u in range(32):
        lo = ((u // 4) * 8 + u % 4) * UNIT
        hi = lo + 4 * UNIT
        parts = []
        for at in (lo, hi):
            part = x_ref[:, at : at + UNIT].astype(F32) * inv * gain_ref[:, at : at + UNIT]
            parts.append(part.astype(BF16))
        own_ref[u] = jnp.where(first, parts[0], parts[1])
        send_ref[u] = jnp.where(first, parts[1], parts[0])


def normalize(core, source, gain):
    tokens, width = source.shape
    step = 32
    return pl.pallas_call(
        norm_kernel,
        grid=(tokens // step,),
        in_specs=[
            pl.BlockSpec(memory_space=pltpu.SMEM),
            pl.BlockSpec((step, width), lambda i: (i, 0)),
            pl.BlockSpec((1, width), lambda i: (0, 0)),
        ],
        out_specs=[
            pl.BlockSpec((32, step, UNIT), lambda i: (0, i, 0)),
            pl.BlockSpec((32, step, UNIT), lambda i: (0, i, 0)),
            pl.BlockSpec((step, UNIT), lambda i: (i, 0)),
        ],
        out_shape=[
            jax.ShapeDtypeStruct((32, tokens, UNIT), BF16),
            jax.ShapeDtypeStruct((32, tokens, UNIT), BF16),
            jax.ShapeDtypeStruct((tokens, UNIT), F32),
        ],
        name="norm",
    )(core, source, gain)


def project_kernel(table_ref, own_ref, other_ref, *refs):
    pieces, (mine_ref, theirs_ref) = refs[:-2], refs[-2:]
    tokens = own_ref.shape[1]
    for side in (0, 1):
        total = None
        for (at_side, first, count), piece in zip(PIECES, pieces):
            if at_side != side:
                continue
            top, low = [], []
            for j in range(count):
                u = table_ref[first + j]
                top.append(own_ref[u])
                low.append(other_ref[u])
            lhs = jnp.concatenate(
                [jnp.concatenate(top, axis=1), jnp.concatenate(low, axis=1)], axis=0
            )
            term = jnp.dot(lhs, piece[...], preferred_element_type=F32)
            total = term if total is None else total + term
        cols = slice(side * total.shape[1], (side + 1) * total.shape[1])
        mine_ref[:, cols] = total[:tokens]
        theirs_ref[:, cols] = total[tokens:]


def project(table, own, other, pieces):
    tokens = own.shape[1]
    width = 2 * pieces[0].shape[1]
    whole = pl.BlockSpec(memory_space=pltpu.VMEM)
    return pl.pallas_call(
        project_kernel,
        in_specs=[pl.BlockSpec(memory_space=pltpu.SMEM)] + [whole] * (2 + len(pieces)),
        out_specs=[whole, whole],
        out_shape=[jax.ShapeDtypeStruct((tokens, width), F32)] * 2,
        compiler_params=pltpu.CompilerParams(vmem_limit_bytes=VMEM_LIMIT),
        name="project",
    )(table, own, other, *pieces)


def attention_kernel(bias_ref, q_ref, go_ref, *refs):
    keys, values = refs[: BACK + 1], refs[BACK + 1 : 2 * BACK + 2]
    att_ref, dq_ref, own_ref = refs[2 * BACK + 2 : 2 * BACK + 5]
    back_refs = refs[2 * BACK + 5 : 3 * BACK + 5]
    probs_ref, grads_ref, q_rows, go_rows = refs[3 * BACK + 5 :]
    head = pl.program_id(0)
    scale = HEAD ** (-0.5)
    group = q_ref.shape[1] // HEAD
    tokens = q_ref.shape[0]
    key = jnp.concatenate([r[...] for r in keys], axis=0)
    value = jnp.concatenate([r[...] for r in values], axis=0)
    key_t = key.astype(F32).T.astype(BF16)
    value_t = value.astype(F32).T.astype(BF16)
    bias = bias_ref[...]
    nt = (((1,), (1,)), ((), ()))
    for j in range(group):
        cols = slice(j * HEAD, (j + 1) * HEAD)
        q = q_ref[:, cols]
        go = go_ref[:, cols]
        q_rows[j * tokens : (j + 1) * tokens, :] = q
        go_rows[j * tokens : (j + 1) * tokens, :] = go
        score = lax.dot_general(key, q, nt, preferred_element_type=F32) * scale + bias
        top = jnp.max(score, axis=0, keepdims=True)
        expo = jnp.exp(score - top)
        total = jnp.sum(expo, axis=0, keepdims=True)
        summed = jnp.dot(value_t, expo.astype(BF16), preferred_element_type=F32) / total
        att = summed.astype(BF16).astype(F32)
        go_t = go.astype(F32).T
        delta = jnp.sum(att * go_t, axis=0, keepdims=True)
        att_ref[:, cols] = att.T.astype(BF16)
        probs = expo * (1.0 / total)
        grad_probs = lax.dot_general(value, go, nt, preferred_element_type=F32)
        grad_scores = (probs * (grad_probs - delta)).astype(BF16)
        probs_ref[:, cols] = probs.astype(BF16)
        grads_ref[:, cols] = grad_scores
        dq = jnp.dot(key_t, grad_scores, preferred_element_type=F32) * scale
        dq_ref[:, cols] = dq.T.astype(BF16)
    grad_key = jnp.dot(grads_ref[...], q_rows[...], preferred_element_type=F32) * scale
    grad_value = jnp.dot(probs_ref[...], go_rows[...], preferred_element_type=F32)
    kv_width = own_ref.shape[1] // 2
    key_at = pl.multiple_of(head * HEAD, HEAD)
    value_at = pl.multiple_of(kv_width + head * HEAD, HEAD)
    own_ref[:, pl.ds(key_at, HEAD)] = grad_key[:tokens]
    own_ref[:, pl.ds(value_at, HEAD)] = grad_value[:tokens]
    for k, ref in enumerate(back_refs):
        at = slice((k + 1) * tokens, (k + 2) * tokens)
        ref[:, pl.ds(key_at, HEAD)] = grad_key[at].astype(BF16)
        ref[:, pl.ds(value_at, HEAD)] = grad_value[at].astype(BF16)


def attention(bias, queries, grad_out, kv_blocks):
    tokens, q_width = queries.shape
    kv_total = kv_blocks[0].shape[1]
    kv_heads = kv_total // 2 // HEAD
    group_cols = q_width // kv_heads
    span = (BACK + 1) * tokens
    q_spec = pl.BlockSpec((tokens, group_cols), lambda h: (0, h))
    key_spec = pl.BlockSpec((tokens, HEAD), lambda h: (0, h))
    value_spec = pl.BlockSpec((tokens, HEAD), lambda h: (0, kv_heads + h))
    grad_spec = pl.BlockSpec((tokens, kv_total), lambda h: (0, 0))
    return pl.pallas_call(
        attention_kernel,
        grid=(kv_heads,),
        in_specs=[pl.BlockSpec((span, tokens), lambda h: (0, 0)), q_spec, q_spec]
        + [key_spec] * (BACK + 1)
        + [value_spec] * (BACK + 1),
        out_specs=[q_spec, q_spec] + [grad_spec] * (BACK + 1),
        out_shape=[
            jax.ShapeDtypeStruct((tokens, q_width), BF16),
            jax.ShapeDtypeStruct((tokens, q_width), BF16),
            jax.ShapeDtypeStruct((tokens, kv_total), F32),
        ]
        + [jax.ShapeDtypeStruct((tokens, kv_total), BF16)] * BACK,
        scratch_shapes=[
            pltpu.VMEM((span, group_cols), BF16),
            pltpu.VMEM((span, group_cols), BF16),
            pltpu.VMEM((tokens * group_cols // HEAD, HEAD), BF16),
            pltpu.VMEM((tokens * group_cols // HEAD, HEAD), BF16),
        ],
        compiler_params=pltpu.CompilerParams(vmem_limit_bytes=VMEM_LIMIT),
        name="attention",
    )(bias, queries, grad_out, *kv_blocks, *kv_blocks)


def grad_normed_kernel(table_ref, mine_ref, theirs_ref, *refs):
    pieces, (own_ref, send_ref, acc_ref) = refs[:-3], refs[-3:]
    tokens = mine_ref.shape[0]
    nt = (((1,), (1,)), ((), ()))
    for (side, first, count), piece in zip(PIECES, pieces):
        width = piece.shape[1]
        cols = slice(side * width, (side + 1) * width)
        lhs = jnp.concatenate([mine_ref[:, cols], theirs_ref[:, cols]], axis=0)
        term = lax.dot_general(lhs, piece[...], nt, preferred_element_type=F32)
        for j in range(count):
            u = table_ref[first + j]
            part = term[:, j * UNIT : (j + 1) * UNIT]
            if side == 0:
                acc_ref[u] = part
            else:
                part = (part + acc_ref[u]).astype(BF16)
                own_ref[u] = part[:tokens]
                send_ref[u] = part[tokens:]


def grad_normed(table, mine, theirs, pieces):
    tokens = mine.shape[0]
    whole = pl.BlockSpec(memory_space=pltpu.VMEM)
    return pl.pallas_call(
        grad_normed_kernel,
        in_specs=[pl.BlockSpec(memory_space=pltpu.SMEM)] + [whole] * (2 + len(pieces)),
        out_specs=[whole, whole],
        out_shape=[jax.ShapeDtypeStruct((32, tokens, UNIT), BF16)] * 2,
        scratch_shapes=[pltpu.VMEM((32, 2 * tokens, UNIT), F32)],
        compiler_params=pltpu.CompilerParams(vmem_limit_bytes=VMEM_LIMIT),
        name="grad_normed",
    )(table, mine, theirs, *pieces)


def norm_back_kernel(core_ref, own_ref, recv_ref, x_ref, inv_ref, gain_ref, out_ref, sum_ref):
    first = core_ref[0] == 0
    inv = inv_ref[:, :1]
    width = x_ref.shape[1]
    step = x_ref.shape[0]

    @pl.when(pl.program_id(0) == 0)
    def _():
        sum_ref[...] = jnp.zeros_like(sum_ref)

    def unit(at):
        u = (at // 8) * 4 + at % 4
        same = first if (at % 8) < 4 else jnp.logical_not(first)
        cols = slice(at * UNIT, (at + 1) * UNIT)
        grad = jnp.where(same, own_ref[u], recv_ref[u]).astype(F32)
        scaled = x_ref[:, cols].astype(F32) * inv
        return cols, grad, scaled

    dots = jnp.zeros((step, UNIT), F32)
    for at in range(width // UNIT):
        cols, grad, scaled = unit(at)
        both = grad * scaled
        sum_ref[:, cols] += jnp.sum(both.reshape(step // 8, 8, UNIT), axis=0)
        dots += both * gain_ref[:, cols]
    mean = jnp.sum(dots, axis=1, keepdims=True) * (1.0 / width)
    for at in range(width // UNIT):
        cols, grad, scaled = unit(at)
        out_ref[:, cols] = (inv * (grad * gain_ref[:, cols] - scaled * mean)).astype(BF16)


def norm_back(core, own, recv, source, inv, gain):
    tokens, width = source.shape
    step = 32
    unit_spec = pl.BlockSpec((32, step, UNIT), lambda i: (0, i, 0))
    return pl.pallas_call(
        norm_back_kernel,
        grid=(tokens // step,),
        in_specs=[
            pl.BlockSpec(memory_space=pltpu.SMEM),
            unit_spec,
            unit_spec,
            pl.BlockSpec((step, width), lambda i: (i, 0)),
            pl.BlockSpec((step, UNIT), lambda i: (i, 0)),
            pl.BlockSpec((1, width), lambda i: (0, 0)),
        ],
        out_specs=[
            pl.BlockSpec((step, width), lambda i: (i, 0)),
            pl.BlockSpec((8, width), lambda i: (0, 0)),
        ],
        out_shape=[
            jax.ShapeDtypeStruct((tokens, width), BF16),
            jax.ShapeDtypeStruct((8, width), F32),
        ],
        name="norm_back",
    )(core, own, recv, source, inv, gain)


def grad_weight_kernel(*refs):
    columns, grads, out_ref = refs[:8], refs[8:16], refs[16]
    grad = jnp.concatenate([g[...] for g in grads], axis=0)
    for j in range(0, columns[0].shape[0], 2):
        lhs = jnp.concatenate(
            [jnp.concatenate([c[j], c[j + 1]], axis=1) for c in columns], axis=0
        )
        part = lax.dot_general(
            lhs, grad, (((0,), (0,)), ((), ())), preferred_element_type=F32
        ).astype(BF16)
        out_ref[j] = part[:UNIT]
        out_ref[j + 1] = part[UNIT:]


def grad_weight_part(columns, grads):
    units, width = columns[0].shape[0], grads[0].shape[1]
    whole = pl.BlockSpec(memory_space=pltpu.VMEM)
    return pl.pallas_call(
        grad_weight_kernel,
        in_specs=[whole] * 16,
        out_specs=whole,
        out_shape=jax.ShapeDtypeStruct((units, UNIT, width), BF16),
        compiler_params=pltpu.CompilerParams(vmem_limit_bytes=VMEM_LIMIT),
        name="grad_weight",
    )(*columns, *grads)


def sum_everywhere(value):
    for axis in ("core", "zlo", "zhi"):
        value = value + shift(value, axis, 1)
    for axis in ("y", "x"):
        value = value + shift(value, axis, 1) + shift(value, axis, 2) + shift(value, axis, 3)
    return value


def shards(layer_input, queries, grad_out, segment_ids, kv_weight, norm_gain):
    source = layer_input[0]
    tokens = source.shape[0]
    core = lax.axis_index("core").astype(jnp.int32)[None]
    place = lax.axis_index("x") * SIZES["zhi"] + lax.axis_index("zhi")
    gain = norm_gain[None]
    table = unit_table()

    doc = segment_ids[0]
    docs = [doc] + [
        jnp.where(place >= k, shift_seq(doc, k), -1) for k in range(1, BACK + 1)
    ]
    local = jnp.arange(tokens, dtype=jnp.int32)
    causal = rows([local] + [jnp.full((tokens,), -1, jnp.int32)] * BACK)
    allowed = (rows(docs)[:, None] == doc[None, :]) & (causal[:, None] <= local[None, :])
    bias = jnp.where(allowed, 0.0, -1e30).astype(F32)

    left, right = gather_weight(kv_weight)
    pieces = left + right
    own, send, inv = normalize(core, source, gain)
    other = shift(send, "core", 1)

    kv_mine, kv_theirs = project(table, own, other, pieces)
    kv_own = (kv_mine + shift(kv_theirs, "core", 1)).astype(BF16)

    def column_block(by):
        at = (lax.axis_index("x") + by) % 4
        return [
            lax.dynamic_index_in_dim(n.reshape(8, 4, tokens, UNIT), at, 1, keepdims=False)
            for n in (own, other)
        ]

    columns = []
    for by in range(4):
        columns += [shift(block, "x", by) if by else block for block in column_block(by)]

    kv_blocks = [kv_own] + [shift_seq(kv_own, k) for k in range(1, BACK + 1)]
    attended, grad_queries, grad_here, *grad_back = attention(
        bias, queries[0], grad_out[0], kv_blocks
    )
    total = grad_here
    for k, part in enumerate(grad_back):
        total = total + shift_seq(part, -(k + 1)).astype(F32)
    grad_own = total.astype(BF16)
    grad_other = shift(grad_own, "core", 1)

    grads = [grad_own, grad_other]
    for by in range(1, 4):
        far = shift(grad_own, "x", by)
        grads += [far, shift(far, "core", 1)]

    mine, theirs = grad_normed(table, grad_own, grad_other, pieces)
    grad_input, gain_rows = norm_back(
        core, mine, shift(theirs, "core", 1), source, inv, gain
    )
    grad_gain = sum_everywhere(jnp.sum(gain_rows, axis=0))

    partial = grad_weight_part(columns, grads).reshape(16, 64, kv_weight.shape[1])
    arrived = lax.all_to_all(partial, ("zlo", "y", "zhi"), 0, 0, tiled=True)
    grad_weight = jnp.sum(arrived.astype(F32), axis=0)
    return attended[None], grad_queries[None], grad_input[None], grad_weight, grad_gain


def solution(mesh):
    fine = Mesh(mesh.devices.reshape(tuple(SIZES.values())), tuple(SIZES))
    tokens = P(BLK, SEQ, None)
    weight = P(BLK + SEQ, None)
    return jax.shard_map(
        shards,
        mesh=fine,
        in_specs=(tokens, tokens, tokens, P(BLK, SEQ), weight, P()),
        out_specs=(tokens, tokens, tokens, weight, P()),
        check_vma=False,
    )
```

```python
import jax
import jax.numpy as jnp
from jax import lax
from jax.experimental import pallas as pl
from jax.experimental.pallas import tpu as pltpu
from jax.sharding import Mesh, PartitionSpec as P


HEAD = 128
UNIT = 128
BACK = 4
EPSILON = 1e-05
BF16 = jnp.bfloat16
F32 = jnp.float32
VMEM_LIMIT = 56 * 1024 * 1024

SIZES = {"zlo": 2, "y": 4, "core": 2, "x": 4, "zhi": 2}
BLK = ("zlo", "y", "core")
SEQ = ("x", "zhi")
REL4 = (0, -1, 1, 2)


def shift(value, axis, by):
    n = SIZES[axis]
    return lax.ppermute(value, axis, [(i, (i + by) % n) for i in range(n)])


def shift_seq(value, by):
    n = SIZES["x"] * SIZES["zhi"]
    pairs = [(i, i + by) for i in range(n) if 0 <= i + by < n]
    return lax.ppermute(value, SEQ, pairs)


def rows(pieces):
    return jnp.concatenate(pieces, axis=0)


def ring4(value, axis):
    half = value.shape[0] // 2
    before = shift(value, axis, 1)
    after = shift(value, axis, -1)
    return [value, before, after, shift(before[:half], axis, 1), shift(after[half:], axis, -1)]


def ring4_halves(first, second, axis):
    before_first = shift(first, axis, 1)
    after_second = shift(second, axis, -1)
    before_second = shift(second, axis, 1)
    after_first = shift(first, axis, -1)
    far_first = shift(before_first, axis, 1)
    far_second = shift(after_second, axis, -1)
    near = [first, second, before_first, before_second, after_first, after_second]
    return near, [far_first, far_second]


def join_kernel(*refs):
    pieces, (first_ref, second_ref, sems) = refs[:5], refs[5:]
    size = pieces[0].shape[0]
    copies = []
    for i, piece in enumerate(pieces):
        n = piece.shape[0]
        out = first_ref if i < 2 else second_ref
        at = (0, size, 0, size, size + n)[i]
        copies.append(pltpu.make_async_copy(piece, out.at[pl.ds(at, n)], sems.at[i]))
    for copy in copies:
        copy.start()
    for copy in copies:
        copy.wait()


def join(pieces):
    size, width = pieces[0].shape
    anywhere = pl.BlockSpec(memory_space=pl.ANY)
    return pl.pallas_call(
        join_kernel,
        in_specs=[anywhere] * 5,
        out_specs=[anywhere] * 2,
        out_shape=[jax.ShapeDtypeStruct((2 * size, width), BF16)] * 2,
        scratch_shapes=[pltpu.SemaphoreType.DMA((5,))],
        name="join",
    )(*pieces)


def gather_weight(weight):
    other = shift(weight, "zhi", 1)
    across = shift(weight, "zlo", 1)
    both = lax.ppermute(weight, ("zlo", "zhi"), [(i, 3 - i) for i in range(4)])
    pair = jnp.where(
        lax.axis_index("zhi") == 0,
        rows([weight, other, across, both]),
        rows([other, weight, both, across]),
    )
    half = pair.shape[1] // 2
    left = ring4(pair[:, :half], "y")
    right = ring4(pair[:, half:], "x")
    left_near, left_far = ring4_halves(*join(left), "x")
    right_near, right_far = ring4_halves(*join(right), "y")
    return left_near + right_near, left_far + right_far


def unit_table():
    zlo, y, x = lax.axis_index("zlo"), lax.axis_index("y"), lax.axis_index("x")
    rel = jnp.array(REL4, jnp.int32)
    zs = (zlo + jnp.arange(2, dtype=jnp.int32)) % 2
    ys, xs = (y + rel) % 4, (x + rel) % 4
    left = xs[:, None, None] * 8 + zs[None, None, :] * 4 + ys[None, :, None]
    right = xs[None, :, None] * 8 + zs[None, None, :] * 4 + ys[:, None, None]
    return jnp.stack([left, right]).reshape(64).astype(jnp.int32)


NEAR = tuple((side, side * 32 + first) for side in (0, 1) for first in (0, 4, 8, 12, 16, 20))
FAR = tuple((side, side * 32 + first) for side in (0, 1) for first in (24, 28))
COUNT = 4


def norm_kernel(core_ref, x_ref, gain_ref, own_ref, send_ref, inv_ref):
    source = x_ref[...].astype(F32)
    inv = lax.rsqrt(jnp.mean(source * source, axis=1, keepdims=True) + EPSILON)
    inv_ref[...] = jnp.broadcast_to(inv, inv_ref.shape)
    first = core_ref[0] == 0
    for u in range(32):
        lo = ((u % 8) * 8 + u // 8) * UNIT
        hi = lo + 4 * UNIT
        parts = []
        for at in (lo, hi):
            part = x_ref[:, at : at + UNIT].astype(F32) * inv * gain_ref[:, at : at + UNIT]
            parts.append(part.astype(BF16))
        own_ref[u] = jnp.where(first, parts[0], parts[1])
        send_ref[u] = jnp.where(first, parts[1], parts[0])


def normalize(core, source, gain):
    tokens, width = source.shape
    step = 32
    return pl.pallas_call(
        norm_kernel,
        grid=(tokens // step,),
        in_specs=[
            pl.BlockSpec(memory_space=pltpu.SMEM),
            pl.BlockSpec((step, width), lambda i: (i, 0)),
            pl.BlockSpec((1, width), lambda i: (0, 0)),
        ],
        out_specs=[
            pl.BlockSpec((32, step, UNIT), lambda i: (0, i, 0)),
            pl.BlockSpec((32, step, UNIT), lambda i: (0, i, 0)),
            pl.BlockSpec((step, UNIT), lambda i: (i, 0)),
        ],
        out_shape=[
            jax.ShapeDtypeStruct((32, tokens, UNIT), BF16),
            jax.ShapeDtypeStruct((32, tokens, UNIT), BF16),
            jax.ShapeDtypeStruct((tokens, UNIT), F32),
        ],
        name="norm",
    )(core, source, gain)


def spread_kernel(x_ref, own_ref, other_ref, *refs):
    outs, sems = refs[:4], refs[4]
    copies = []
    for by, out in enumerate(outs):
        at = lax.rem(x_ref[0] + by, 4) * 8
        for i, source in enumerate((own_ref, other_ref)):
            copies.append(
                pltpu.make_async_copy(source.at[pl.ds(at, 8)], out.at[i], sems.at[2 * by + i])
            )
    for copy in copies:
        copy.start()
    for copy in copies:
        copy.wait()


def spread(x, own, other):
    tokens = own.shape[1]
    anywhere = pl.BlockSpec(memory_space=pl.ANY)
    return pl.pallas_call(
        spread_kernel,
        in_specs=[pl.BlockSpec(memory_space=pltpu.SMEM), anywhere, anywhere],
        out_specs=[anywhere] * 4,
        out_shape=[jax.ShapeDtypeStruct((2, 8, tokens, UNIT), BF16)] * 4,
        scratch_shapes=[pltpu.SemaphoreType.DMA((8,))],
        name="spread",
    )(x, own, other)


def project_sum(table_ref, own_ref, other_ref, pieces, refs, side):
    total = None
    for (at_side, first), piece in zip(pieces, refs):
        if at_side != side:
            continue
        top = [own_ref[table_ref[first + j]] for j in range(COUNT)]
        low = [other_ref[table_ref[first + j]] for j in range(COUNT)]
        lhs = jnp.concatenate(
            [jnp.concatenate(top, axis=1), jnp.concatenate(low, axis=1)], axis=0
        )
        term = jnp.dot(lhs, piece[...], preferred_element_type=F32)
        total = term if total is None else total + term
    return total


def project_near_kernel(table_ref, own_ref, other_ref, *refs):
    out_ref = refs[-1]
    for side in (0, 1):
        total = project_sum(table_ref, own_ref, other_ref, NEAR, refs[:-1], side)
        width = total.shape[1]
        out_ref[:, side * width : (side + 1) * width] = total


def project_near(table, own, other, pieces):
    tokens = own.shape[1]
    width = 2 * pieces[0].shape[1]
    whole = pl.BlockSpec(memory_space=pltpu.VMEM)
    return pl.pallas_call(
        project_near_kernel,
        in_specs=[pl.BlockSpec(memory_space=pltpu.SMEM)] + [whole] * (2 + len(pieces)),
        out_specs=whole,
        out_shape=jax.ShapeDtypeStruct((2 * tokens, width), F32),
        compiler_params=pltpu.CompilerParams(vmem_limit_bytes=VMEM_LIMIT),
        name="project_near",
    )(table, own, other, *pieces)


def project_far_kernel(table_ref, own_ref, other_ref, near_ref, *refs):
    pieces, (mine_ref, theirs_ref) = refs[:-2], refs[-2:]
    tokens = own_ref.shape[1]
    for side in (0, 1):
        total = project_sum(table_ref, own_ref, other_ref, FAR, pieces, side)
        width = total.shape[1]
        cols = slice(side * width, (side + 1) * width)
        total = total + near_ref[:, cols]
        mine_ref[:, cols] = total[:tokens]
        theirs_ref[:, cols] = total[tokens:]


def project_far(table, own, other, near, pieces):
    tokens = own.shape[1]
    whole = pl.BlockSpec(memory_space=pltpu.VMEM)
    return pl.pallas_call(
        project_far_kernel,
        in_specs=[pl.BlockSpec(memory_space=pltpu.SMEM)] + [whole] * (3 + len(pieces)),
        out_specs=[whole, whole],
        out_shape=[jax.ShapeDtypeStruct((tokens, near.shape[1]), F32)] * 2,
        compiler_params=pltpu.CompilerParams(vmem_limit_bytes=VMEM_LIMIT),
        name="project_far",
    )(table, own, other, near, *pieces)


def attention_kernel(bias_ref, q_ref, go_ref, *refs):
    keys, values = refs[: BACK + 1], refs[BACK + 1 : 2 * BACK + 2]
    att_ref, dq_ref, own_ref = refs[2 * BACK + 2 : 2 * BACK + 5]
    back_refs = refs[2 * BACK + 5 : 3 * BACK + 5]
    probs_ref, grads_ref, q_rows, go_rows = refs[3 * BACK + 5 :]
    head = pl.program_id(0)
    scale = HEAD ** (-0.5)
    group = q_ref.shape[1] // HEAD
    tokens = q_ref.shape[0]
    key = jnp.concatenate([r[...] for r in keys], axis=0)
    value = jnp.concatenate([r[...] for r in values], axis=0)
    key_t = key.astype(F32).T.astype(BF16)
    value_t = value.astype(F32).T.astype(BF16)
    bias = bias_ref[...]
    nt = (((1,), (1,)), ((), ()))
    for j in range(group):
        cols = slice(j * HEAD, (j + 1) * HEAD)
        q = q_ref[:, cols]
        go = go_ref[:, cols]
        q_rows[j * tokens : (j + 1) * tokens, :] = q
        go_rows[j * tokens : (j + 1) * tokens, :] = go
        score = lax.dot_general(key, q, nt, preferred_element_type=F32) * scale + bias
        top = jnp.max(score, axis=0, keepdims=True)
        expo = jnp.exp(score - top)
        total = jnp.sum(expo, axis=0, keepdims=True)
        summed = jnp.dot(value_t, expo.astype(BF16), preferred_element_type=F32) / total
        att = summed.astype(BF16).astype(F32)
        go_t = go.astype(F32).T
        delta = jnp.sum(att * go_t, axis=0, keepdims=True)
        att_ref[:, cols] = att.T.astype(BF16)
        probs = expo * (1.0 / total)
        grad_probs = lax.dot_general(value, go, nt, preferred_element_type=F32)
        grad_scores = (probs * (grad_probs - delta)).astype(BF16)
        probs_ref[:, cols] = probs.astype(BF16)
        grads_ref[:, cols] = grad_scores
        dq = jnp.dot(key_t, grad_scores, preferred_element_type=F32) * scale
        dq_ref[:, cols] = dq.T.astype(BF16)
    grad_key = jnp.dot(grads_ref[...], q_rows[...], preferred_element_type=F32) * scale
    grad_value = jnp.dot(probs_ref[...], go_rows[...], preferred_element_type=F32)
    kv_width = own_ref.shape[1] // 2
    key_at = pl.multiple_of(head * HEAD, HEAD)
    value_at = pl.multiple_of(kv_width + head * HEAD, HEAD)
    own_ref[:, pl.ds(key_at, HEAD)] = grad_key[:tokens]
    own_ref[:, pl.ds(value_at, HEAD)] = grad_value[:tokens]
    for k, ref in enumerate(back_refs):
        at = slice((k + 1) * tokens, (k + 2) * tokens)
        ref[:, pl.ds(key_at, HEAD)] = grad_key[at].astype(BF16)
        ref[:, pl.ds(value_at, HEAD)] = grad_value[at].astype(BF16)


def attention(bias, queries, grad_out, kv_blocks):
    tokens, q_width = queries.shape
    kv_total = kv_blocks[0].shape[1]
    kv_heads = kv_total // 2 // HEAD
    group_cols = q_width // kv_heads
    span = (BACK + 1) * tokens
    q_spec = pl.BlockSpec((tokens, group_cols), lambda h: (0, h))
    key_spec = pl.BlockSpec((tokens, HEAD), lambda h: (0, h))
    value_spec = pl.BlockSpec((tokens, HEAD), lambda h: (0, kv_heads + h))
    grad_spec = pl.BlockSpec((tokens, kv_total), lambda h: (0, 0))
    return pl.pallas_call(
        attention_kernel,
        grid=(kv_heads,),
        in_specs=[pl.BlockSpec((span, tokens), lambda h: (0, 0)), q_spec, q_spec]
        + [key_spec] * (BACK + 1)
        + [value_spec] * (BACK + 1),
        out_specs=[q_spec, q_spec] + [grad_spec] * (BACK + 1),
        out_shape=[
            jax.ShapeDtypeStruct((tokens, q_width), BF16),
            jax.ShapeDtypeStruct((tokens, q_width), BF16),
            jax.ShapeDtypeStruct((tokens, kv_total), F32),
        ]
        + [jax.ShapeDtypeStruct((tokens, kv_total), BF16)] * BACK,
        scratch_shapes=[
            pltpu.VMEM((span, group_cols), BF16),
            pltpu.VMEM((span, group_cols), BF16),
            pltpu.VMEM((tokens * group_cols // HEAD, HEAD), BF16),
            pltpu.VMEM((tokens * group_cols // HEAD, HEAD), BF16),
        ],
        compiler_params=pltpu.CompilerParams(vmem_limit_bytes=VMEM_LIMIT),
        name="attention",
    )(bias, queries, grad_out, *kv_blocks, *kv_blocks)


def grad_normed_kernel(table_ref, mine_ref, theirs_ref, *refs):
    pieces, (own_ref, send_ref, acc_ref) = refs[:-3], refs[-3:]
    tokens = mine_ref.shape[0]
    nt = (((1,), (1,)), ((), ()))
    order = sorted(zip(NEAR + FAR, pieces), key=lambda entry: entry[0])
    for (side, first), piece in order:
        width = piece.shape[1]
        cols = slice(side * width, (side + 1) * width)
        lhs = jnp.concatenate([mine_ref[:, cols], theirs_ref[:, cols]], axis=0)
        term = lax.dot_general(lhs, piece[...], nt, preferred_element_type=F32)
        for j in range(COUNT):
            u = table_ref[first + j]
            part = term[:, j * UNIT : (j + 1) * UNIT]
            if side == 0:
                acc_ref[u] = part
            else:
                part = (part + acc_ref[u]).astype(BF16)
                own_ref[u] = part[:tokens]
                send_ref[u] = part[tokens:]


def grad_normed(table, mine, theirs, pieces):
    tokens = mine.shape[0]
    whole = pl.BlockSpec(memory_space=pltpu.VMEM)
    return pl.pallas_call(
        grad_normed_kernel,
        in_specs=[pl.BlockSpec(memory_space=pltpu.SMEM)] + [whole] * (2 + len(pieces)),
        out_specs=[whole, whole],
        out_shape=[jax.ShapeDtypeStruct((32, tokens, UNIT), BF16)] * 2,
        scratch_shapes=[pltpu.VMEM((32, 2 * tokens, UNIT), F32)],
        compiler_params=pltpu.CompilerParams(vmem_limit_bytes=VMEM_LIMIT),
        name="grad_normed",
    )(table, mine, theirs, *pieces)


def norm_back_kernel(core_ref, own_ref, recv_ref, x_ref, inv_ref, gain_ref, out_ref, sum_ref):
    first = core_ref[0] == 0
    inv = inv_ref[:, :1]
    width = x_ref.shape[1]
    step = x_ref.shape[0]

    @pl.when(pl.program_id(0) == 0)
    def _():
        sum_ref[...] = jnp.zeros_like(sum_ref)

    def unit(at):
        u = (at % 4) * 8 + at // 8
        same = first if (at % 8) < 4 else jnp.logical_not(first)
        cols = slice(at * UNIT, (at + 1) * UNIT)
        grad = jnp.where(same, own_ref[u], recv_ref[u]).astype(F32)
        scaled = x_ref[:, cols].astype(F32) * inv
        return cols, grad, scaled

    dots = jnp.zeros((step, UNIT), F32)
    for at in range(width // UNIT):
        cols, grad, scaled = unit(at)
        both = grad * scaled
        sum_ref[:, cols] += jnp.sum(both.reshape(step // 8, 8, UNIT), axis=0)
        dots += both * gain_ref[:, cols]
    mean = jnp.sum(dots, axis=1, keepdims=True) * (1.0 / width)
    for at in range(width // UNIT):
        cols, grad, scaled = unit(at)
        out_ref[:, cols] = (inv * (grad * gain_ref[:, cols] - scaled * mean)).astype(BF16)


def norm_back(core, own, recv, source, inv, gain):
    tokens, width = source.shape
    step = 32
    unit_spec = pl.BlockSpec((32, step, UNIT), lambda i: (0, i, 0))
    return pl.pallas_call(
        norm_back_kernel,
        grid=(tokens // step,),
        in_specs=[
            pl.BlockSpec(memory_space=pltpu.SMEM),
            unit_spec,
            unit_spec,
            pl.BlockSpec((step, width), lambda i: (i, 0)),
            pl.BlockSpec((step, UNIT), lambda i: (i, 0)),
            pl.BlockSpec((1, width), lambda i: (0, 0)),
        ],
        out_specs=[
            pl.BlockSpec((step, width), lambda i: (i, 0)),
            pl.BlockSpec((8, width), lambda i: (0, 0)),
        ],
        out_shape=[
            jax.ShapeDtypeStruct((tokens, width), BF16),
            jax.ShapeDtypeStruct((8, width), F32),
        ],
        name="norm_back",
    )(core, own, recv, source, inv, gain)


def grad_weight_kernel(*refs):
    columns, grads, out_ref = refs[:4], refs[4:12], refs[12]
    grad = jnp.concatenate([g[...] for g in grads], axis=0)
    for j in range(0, columns[0].shape[1], 2):
        lhs = jnp.concatenate(
            [
                jnp.concatenate([c[i, j], c[i, j + 1]], axis=1)
                for c in columns
                for i in (0, 1)
            ],
            axis=0,
        )
        part = lax.dot_general(
            lhs, grad, (((0,), (0,)), ((), ())), preferred_element_type=F32
        ).astype(BF16)
        out_ref[j] = part[:UNIT]
        out_ref[j + 1] = part[UNIT:]


def grad_weight_part(columns, grads):
    units, width = columns[0].shape[1], grads[0].shape[1]
    whole = pl.BlockSpec(memory_space=pltpu.VMEM)
    return pl.pallas_call(
        grad_weight_kernel,
        in_specs=[whole] * 12,
        out_specs=whole,
        out_shape=jax.ShapeDtypeStruct((units, UNIT, width), BF16),
        compiler_params=pltpu.CompilerParams(vmem_limit_bytes=VMEM_LIMIT),
        name="grad_weight",
    )(*columns, *grads)


def sum_everywhere(value):
    for axis in ("core", "zlo", "zhi"):
        value = value + shift(value, axis, 1)
    for axis in ("y", "x"):
        value = value + shift(value, axis, 1) + shift(value, axis, 2) + shift(value, axis, 3)
    return value


def step(layer_input, queries, grad_out, segment_ids, kv_weight, norm_gain):
    source = layer_input[0]
    tokens = source.shape[0]
    core = lax.axis_index("core").astype(jnp.int32)[None]
    x = lax.axis_index("x").astype(jnp.int32)[None]
    place = lax.axis_index("x") * SIZES["zhi"] + lax.axis_index("zhi")
    gain = norm_gain[None]
    table = unit_table()

    doc = segment_ids[0]
    moved = [shift_seq(doc, k) for k in range(1, BACK + 1)]
    docs = [doc] + [jnp.where(place > k, d, -1) for k, d in enumerate(moved)]
    local = jnp.arange(tokens, dtype=jnp.int32)
    causal = rows([local] + [jnp.full((tokens,), -1, jnp.int32)] * BACK)
    allowed = (rows(docs)[:, None] == doc[None, :]) & (causal[:, None] <= local[None, :])
    bias = jnp.where(allowed, 0.0, -1e30).astype(F32)

    near, far = gather_weight(kv_weight)
    own, send, inv = normalize(core, source, gain)
    other = shift(send, "core", 1)
    blocks = spread(x, own, other)

    kv_near = project_near(table, own, other, near)
    kv_mine, kv_theirs = project_far(table, own, other, kv_near, far)
    kv_own = (kv_mine + shift(kv_theirs, "core", 1)).astype(BF16)

    kv_blocks = [kv_own] + [shift_seq(kv_own, k) for k in range(1, BACK + 1)]
    columns = [shift(block, "x", by) if by else block for by, block in enumerate(blocks)]
    attended, grad_queries, grad_here, *grad_back = attention(
        bias, queries[0], grad_out[0], kv_blocks
    )
    total = grad_here
    for k, part in enumerate(grad_back):
        total = total + shift_seq(part, -(k + 1)).astype(F32)
    grad_own = total.astype(BF16)
    grad_other = shift(grad_own, "core", 1)
    grads = [grad_own, grad_other]
    fars = [shift(grad_own, "x", by) for by in range(1, 4)]
    for block in fars:
        grads += [block, shift(block, "core", 1)]

    mine, theirs = grad_normed(table, grad_own, grad_other, near + far)
    theirs = shift(theirs, "core", 1)
    grad_input, gain_rows = norm_back(core, mine, theirs, source, inv, gain)
    partial = grad_weight_part(columns, grads).reshape(16, 64, kv_weight.shape[1])
    arrived = lax.all_to_all(partial, ("zlo", "y", "zhi"), 0, 0, tiled=True)
    grad_weight = jnp.sum(arrived.astype(F32), axis=0)
    grad_gain = sum_everywhere(jnp.sum(gain_rows, axis=0))
    return attended[None], grad_queries[None], grad_input[None], grad_weight, grad_gain


def solution(mesh):
    fine = Mesh(mesh.devices.reshape(tuple(SIZES.values())), tuple(SIZES))
    tokens = P(BLK, SEQ, None)
    weight = P(BLK + SEQ, None)
    return jax.shard_map(
        step,
        mesh=fine,
        in_specs=(tokens, tokens, tokens, P(BLK, SEQ), weight, P()),
        out_specs=(tokens, tokens, tokens, weight, P()),
        check_vma=False,
    )
```

```python
import jax
import jax.numpy as jnp
from jax import lax
from jax.experimental import pallas as pl
from jax.experimental.pallas import tpu as pltpu
from jax.sharding import Mesh, PartitionSpec as P


HEAD = 128
UNIT = 128
BACK = 4
EPSILON = 1e-05
BF16 = jnp.bfloat16
F32 = jnp.float32
VMEM_LIMIT = 56 * 1024 * 1024

SIZES = {"zlo": 2, "y": 4, "core": 2, "x": 4, "zhi": 2}
BLK = ("zlo", "y", "core")
SEQ = ("x", "zhi")
REL4 = (0, -1, 1, 2)


def shift(value, axis, by):
    n = SIZES[axis]
    return lax.ppermute(value, axis, [(i, (i + by) % n) for i in range(n)])


def shift_seq(value, by):
    n = SIZES["x"] * SIZES["zhi"]
    pairs = [(i, i + by) for i in range(n) if 0 <= i + by < n]
    return lax.ppermute(value, SEQ, pairs)


def rows(pieces):
    return jnp.concatenate(pieces, axis=0)


def ring4(value, axis):
    half = value.shape[0] // 2
    before = shift(value, axis, 1)
    after = shift(value, axis, -1)
    return [value, before, after, shift(before[:half], axis, 1), shift(after[half:], axis, -1)]


def ring4_halves(first, second, axis):
    before_first = shift(first, axis, 1)
    after_second = shift(second, axis, -1)
    before_second = shift(second, axis, 1)
    after_first = shift(first, axis, -1)
    far_first = shift(before_first, axis, 1)
    far_second = shift(after_second, axis, -1)
    near = [first, second, before_first, before_second, after_first, after_second]
    return near, [far_first, far_second]


def join_kernel(*refs):
    pieces, (first_ref, second_ref) = refs[:5], refs[5:]
    size = pieces[0].shape[0]
    half = size // 2
    first_ref[:size, :] = pieces[0][...]
    first_ref[size:, :] = pieces[1][...]
    second_ref[:size, :] = pieces[2][...]
    second_ref[size : size + half, :] = pieces[3][...]
    second_ref[size + half :, :] = pieces[4][...]


def join(pieces):
    size, width = pieces[0].shape
    whole = pl.BlockSpec(memory_space=pltpu.VMEM)
    return pl.pallas_call(
        join_kernel,
        in_specs=[whole] * 5,
        out_specs=[whole] * 2,
        out_shape=[jax.ShapeDtypeStruct((2 * size, width), BF16)] * 2,
        name="join",
    )(*pieces)


def gather_weight(weight):
    other = shift(weight, "zhi", 1)
    across = shift(weight, "zlo", 1)
    both = lax.ppermute(weight, ("zlo", "zhi"), [(i, 3 - i) for i in range(4)])
    pair = jnp.where(
        lax.axis_index("zhi") == 0,
        rows([weight, other, across, both]),
        rows([other, weight, both, across]),
    )
    half = pair.shape[1] // 2
    left = ring4(pair[:, :half], "y")
    right = ring4(pair[:, half:], "x")
    left_near, left_far = ring4_halves(*join(left), "x")
    right_near, right_far = ring4_halves(*join(right), "y")
    return left_near + right_near, left_far + right_far


def unit_table():
    zlo, y, x = lax.axis_index("zlo"), lax.axis_index("y"), lax.axis_index("x")
    rel = jnp.array(REL4, jnp.int32)
    zs = (zlo + jnp.arange(2, dtype=jnp.int32)) % 2
    ys, xs = (y + rel) % 4, (x + rel) % 4
    left = xs[:, None, None] * 8 + zs[None, None, :] * 4 + ys[None, :, None]
    right = xs[None, :, None] * 8 + zs[None, None, :] * 4 + ys[:, None, None]
    return jnp.stack([left, right]).reshape(64).astype(jnp.int32)


NEAR = tuple((side, side * 32 + first) for side in (0, 1) for first in (0, 4, 8, 12, 16, 20))
FAR = tuple((side, side * 32 + first) for side in (0, 1) for first in (24, 28))
COUNT = 4


def norm_kernel(core_ref, x_ref, gain_ref, own_ref, send_ref, inv_ref):
    source = x_ref[...].astype(F32)
    inv = lax.rsqrt(jnp.mean(source * source, axis=1, keepdims=True) + EPSILON)
    inv_ref[...] = jnp.broadcast_to(inv, inv_ref.shape)
    first = core_ref[0] == 0
    for u in range(32):
        lo = ((u % 8) * 8 + u // 8) * UNIT
        hi = lo + 4 * UNIT
        parts = []
        for at in (lo, hi):
            part = x_ref[:, at : at + UNIT].astype(F32) * inv * gain_ref[:, at : at + UNIT]
            parts.append(part.astype(BF16))
        own_ref[u] = jnp.where(first, parts[0], parts[1])
        send_ref[u] = jnp.where(first, parts[1], parts[0])


def normalize(core, source, gain):
    tokens, width = source.shape
    step = 32
    return pl.pallas_call(
        norm_kernel,
        grid=(tokens // step,),
        in_specs=[
            pl.BlockSpec(memory_space=pltpu.SMEM),
            pl.BlockSpec((step, width), lambda i: (i, 0)),
            pl.BlockSpec((1, width), lambda i: (0, 0)),
        ],
        out_specs=[
            pl.BlockSpec((32, step, UNIT), lambda i: (0, i, 0)),
            pl.BlockSpec((32, step, UNIT), lambda i: (0, i, 0)),
            pl.BlockSpec((step, UNIT), lambda i: (i, 0)),
        ],
        out_shape=[
            jax.ShapeDtypeStruct((32, tokens, UNIT), BF16),
            jax.ShapeDtypeStruct((32, tokens, UNIT), BF16),
            jax.ShapeDtypeStruct((tokens, UNIT), F32),
        ],
        name="norm",
    )(core, source, gain)


def spread_kernel(x_ref, own_ref, other_ref, *outs):
    for by, out in enumerate(outs):
        at = lax.rem(x_ref[0] + by, 4) * 8
        out[0] = own_ref[pl.ds(at, 8)]
        out[1] = other_ref[pl.ds(at, 8)]


def spread(x, own, other):
    tokens = own.shape[1]
    whole = pl.BlockSpec(memory_space=pltpu.VMEM)
    return pl.pallas_call(
        spread_kernel,
        in_specs=[pl.BlockSpec(memory_space=pltpu.SMEM), whole, whole],
        out_specs=[whole] * 4,
        out_shape=[jax.ShapeDtypeStruct((2, 8, tokens, UNIT), BF16)] * 4,
        name="spread",
    )(x, own, other)


def project_sum(table_ref, own_ref, other_ref, pieces, refs, side):
    total = None
    for (at_side, first), piece in zip(pieces, refs):
        if at_side != side:
            continue
        top = [own_ref[table_ref[first + j]] for j in range(COUNT)]
        low = [other_ref[table_ref[first + j]] for j in range(COUNT)]
        lhs = jnp.concatenate(
            [jnp.concatenate(top, axis=1), jnp.concatenate(low, axis=1)], axis=0
        )
        term = jnp.dot(lhs, piece[...], preferred_element_type=F32)
        total = term if total is None else total + term
    return total


def project_near_kernel(table_ref, own_ref, other_ref, *refs):
    out_ref = refs[-1]
    for side in (0, 1):
        total = project_sum(table_ref, own_ref, other_ref, NEAR, refs[:-1], side)
        width = total.shape[1]
        out_ref[:, side * width : (side + 1) * width] = total


def project_near(table, own, other, pieces):
    tokens = own.shape[1]
    width = 2 * pieces[0].shape[1]
    whole = pl.BlockSpec(memory_space=pltpu.VMEM)
    return pl.pallas_call(
        project_near_kernel,
        in_specs=[pl.BlockSpec(memory_space=pltpu.SMEM)] + [whole] * (2 + len(pieces)),
        out_specs=whole,
        out_shape=jax.ShapeDtypeStruct((2 * tokens, width), F32),
        compiler_params=pltpu.CompilerParams(vmem_limit_bytes=VMEM_LIMIT),
        name="project_near",
    )(table, own, other, *pieces)


def project_far_kernel(table_ref, own_ref, other_ref, near_ref, *refs):
    pieces, (mine_ref, theirs_ref) = refs[:-2], refs[-2:]
    tokens = own_ref.shape[1]
    for side in (0, 1):
        total = project_sum(table_ref, own_ref, other_ref, FAR, pieces, side)
        width = total.shape[1]
        cols = slice(side * width, (side + 1) * width)
        total = total + near_ref[:, cols]
        mine_ref[:, cols] = total[:tokens]
        theirs_ref[:, cols] = total[tokens:]


def project_far(table, own, other, near, pieces):
    tokens = own.shape[1]
    whole = pl.BlockSpec(memory_space=pltpu.VMEM)
    return pl.pallas_call(
        project_far_kernel,
        in_specs=[pl.BlockSpec(memory_space=pltpu.SMEM)] + [whole] * (3 + len(pieces)),
        out_specs=[whole, whole],
        out_shape=[jax.ShapeDtypeStruct((tokens, near.shape[1]), F32)] * 2,
        compiler_params=pltpu.CompilerParams(vmem_limit_bytes=VMEM_LIMIT),
        name="project_far",
    )(table, own, other, near, *pieces)


def finish_kernel(mine_ref, other_ref, doc_ref, out_ref):
    tokens = mine_ref.shape[0]
    out_ref[:tokens, :] = (mine_ref[...] + other_ref[...]).astype(BF16)
    out_ref[tokens:, :] = jnp.zeros((8, out_ref.shape[1]), BF16)
    out_ref[tokens:, :tokens] = doc_ref[...].astype(BF16)


def finish(mine, other, doc_rows):
    tokens, width = mine.shape
    whole = pl.BlockSpec(memory_space=pltpu.VMEM)
    return pl.pallas_call(
        finish_kernel,
        in_specs=[whole] * 3,
        out_specs=whole,
        out_shape=jax.ShapeDtypeStruct((tokens + 8, width), BF16),
        name="finish",
    )(mine, other, doc_rows)


def attention_kernel(doc_ref, q_ref, go_ref, *refs):
    keys, values = refs[: BACK + 1], refs[BACK + 1 : 2 * BACK + 2]
    docs, refs = refs[2 * BACK + 2 : 3 * BACK + 3], refs[3 * BACK + 3 :]
    att_ref, dq_ref, own_ref = refs[:3]
    back_refs = refs[3 : BACK + 3]
    probs_ref, grads_ref, q_rows, go_rows, bias_ref = refs[BACK + 3 :]
    head = pl.program_id(0)
    scale = HEAD ** (-0.5)
    group = q_ref.shape[1] // HEAD
    tokens = q_ref.shape[0]

    @pl.when(head == 0)
    def _():
        shape = (tokens, tokens)
        later = lax.broadcasted_iota(jnp.int32, shape, 0) > lax.broadcasted_iota(
            jnp.int32, shape, 1
        )
        for k, ref in enumerate(docs):
            of_key = jnp.broadcast_to(ref[:1, :].astype(F32), shape).T
            bias = jnp.where(of_key == doc_ref[...], 0.0, -1e30)
            bias_ref[k * tokens : (k + 1) * tokens, :] = (
                bias if k else jnp.where(later, -1e30, bias)
            )

    key = jnp.concatenate([r[...] for r in keys], axis=0)
    value = jnp.concatenate([r[...] for r in values], axis=0)
    key_t = key.astype(F32).T.astype(BF16)
    value_t = value.astype(F32).T.astype(BF16)
    bias = bias_ref[...]
    nt = (((1,), (1,)), ((), ()))
    for j in range(group):
        cols = slice(j * HEAD, (j + 1) * HEAD)
        q = q_ref[:, cols]
        go = go_ref[:, cols]
        q_rows[j * tokens : (j + 1) * tokens, :] = q
        go_rows[j * tokens : (j + 1) * tokens, :] = go
        score = lax.dot_general(key, q, nt, preferred_element_type=F32) * scale + bias
        top = jnp.max(score, axis=0, keepdims=True)
        expo = jnp.exp(score - top)
        total = jnp.sum(expo, axis=0, keepdims=True)
        summed = jnp.dot(value_t, expo.astype(BF16), preferred_element_type=F32) / total
        att = summed.astype(BF16).astype(F32)
        go_t = go.astype(F32).T
        delta = jnp.sum(att * go_t, axis=0, keepdims=True)
        att_ref[:, cols] = att.T.astype(BF16)
        probs = expo * (1.0 / total)
        grad_probs = lax.dot_general(value, go, nt, preferred_element_type=F32)
        grad_scores = (probs * (grad_probs - delta)).astype(BF16)
        probs_ref[:, cols] = probs.astype(BF16)
        grads_ref[:, cols] = grad_scores
        dq = jnp.dot(key_t, grad_scores, preferred_element_type=F32) * scale
        dq_ref[:, cols] = dq.T.astype(BF16)
    grad_key = jnp.dot(grads_ref[...], q_rows[...], preferred_element_type=F32) * scale
    grad_value = jnp.dot(probs_ref[...], go_rows[...], preferred_element_type=F32)
    kv_width = own_ref.shape[1] // 2
    key_at = pl.multiple_of(head * HEAD, HEAD)
    value_at = pl.multiple_of(kv_width + head * HEAD, HEAD)
    own_ref[:, pl.ds(key_at, HEAD)] = grad_key[:tokens]
    own_ref[:, pl.ds(value_at, HEAD)] = grad_value[:tokens]
    for k, ref in enumerate(back_refs):
        at = slice((k + 1) * tokens, (k + 2) * tokens)
        ref[:, pl.ds(key_at, HEAD)] = grad_key[at].astype(BF16)
        ref[:, pl.ds(value_at, HEAD)] = grad_value[at].astype(BF16)


def attention(doc, queries, grad_out, kv_blocks):
    tokens, q_width = queries.shape
    kv_total = kv_blocks[0].shape[1]
    kv_heads = kv_total // 2 // HEAD
    group_cols = q_width // kv_heads
    span = (BACK + 1) * tokens
    q_spec = pl.BlockSpec((tokens, group_cols), lambda h: (0, h))
    key_spec = pl.BlockSpec((tokens, HEAD), lambda h: (0, h))
    value_spec = pl.BlockSpec((tokens, HEAD), lambda h: (0, kv_heads + h))
    doc_spec = pl.BlockSpec((8, tokens), lambda h: (tokens // 8, 0))
    grad_spec = pl.BlockSpec((tokens, kv_total), lambda h: (0, 0))
    return pl.pallas_call(
        attention_kernel,
        grid=(kv_heads,),
        in_specs=[pl.BlockSpec((1, tokens), lambda h: (0, 0)), q_spec, q_spec]
        + [key_spec] * (BACK + 1)
        + [value_spec] * (BACK + 1)
        + [doc_spec] * (BACK + 1),
        out_specs=[q_spec, q_spec] + [grad_spec] * (BACK + 1),
        out_shape=[
            jax.ShapeDtypeStruct((tokens, q_width), BF16),
            jax.ShapeDtypeStruct((tokens, q_width), BF16),
            jax.ShapeDtypeStruct((tokens, kv_total), F32),
        ]
        + [jax.ShapeDtypeStruct((tokens, kv_total), BF16)] * BACK,
        scratch_shapes=[
            pltpu.VMEM((span, group_cols), BF16),
            pltpu.VMEM((span, group_cols), BF16),
            pltpu.VMEM((tokens * group_cols // HEAD, HEAD), BF16),
            pltpu.VMEM((tokens * group_cols // HEAD, HEAD), BF16),
            pltpu.VMEM((span, tokens), F32),
        ],
        compiler_params=pltpu.CompilerParams(vmem_limit_bytes=VMEM_LIMIT),
        name="attention",
    )(doc, queries, grad_out, *kv_blocks, *kv_blocks, *kv_blocks)


def grad_normed_kernel(table_ref, mine_ref, theirs_ref, *refs):
    pieces, (own_ref, send_ref, acc_ref) = refs[:-3], refs[-3:]
    tokens = mine_ref.shape[0]
    nt = (((1,), (1,)), ((), ()))
    order = sorted(zip(NEAR + FAR, pieces), key=lambda entry: entry[0])
    for (side, first), piece in order:
        width = piece.shape[1]
        cols = slice(side * width, (side + 1) * width)
        lhs = jnp.concatenate([mine_ref[:, cols], theirs_ref[:, cols]], axis=0)
        term = lax.dot_general(lhs, piece[...], nt, preferred_element_type=F32)
        for j in range(COUNT):
            u = table_ref[first + j]
            part = term[:, j * UNIT : (j + 1) * UNIT]
            if side == 0:
                acc_ref[u] = part
            else:
                part = (part + acc_ref[u]).astype(BF16)
                own_ref[u] = part[:tokens]
                send_ref[u] = part[tokens:]


def grad_normed(table, mine, theirs, pieces):
    tokens = mine.shape[0]
    whole = pl.BlockSpec(memory_space=pltpu.VMEM)
    return pl.pallas_call(
        grad_normed_kernel,
        in_specs=[pl.BlockSpec(memory_space=pltpu.SMEM)] + [whole] * (2 + len(pieces)),
        out_specs=[whole, whole],
        out_shape=[jax.ShapeDtypeStruct((32, tokens, UNIT), BF16)] * 2,
        scratch_shapes=[pltpu.VMEM((32, 2 * tokens, UNIT), F32)],
        compiler_params=pltpu.CompilerParams(vmem_limit_bytes=VMEM_LIMIT),
        name="grad_normed",
    )(table, mine, theirs, *pieces)


def norm_back_kernel(core_ref, own_ref, recv_ref, x_ref, inv_ref, gain_ref, out_ref):
    first = core_ref[0] == 0
    inv = inv_ref[:, :1]
    width = x_ref.shape[1]
    step = x_ref.shape[0]

    def unit(at):
        u = (at % 4) * 8 + at // 8
        same = first if (at % 8) < 4 else jnp.logical_not(first)
        cols = slice(at * UNIT, (at + 1) * UNIT)
        grad = jnp.where(same, own_ref[u], recv_ref[u]).astype(F32)
        scaled = x_ref[:, cols].astype(F32) * inv
        return cols, grad, scaled

    dots = jnp.zeros((step, UNIT), F32)
    for at in range(width // UNIT):
        cols, grad, scaled = unit(at)
        dots += grad * gain_ref[:, cols] * scaled
    mean = jnp.sum(dots, axis=1, keepdims=True) * (1.0 / width)
    for at in range(width // UNIT):
        cols, grad, scaled = unit(at)
        out_ref[:, cols] = (inv * (grad * gain_ref[:, cols] - scaled * mean)).astype(BF16)


def norm_back(core, own, recv, source, inv, gain):
    tokens, width = source.shape
    step = 32
    unit_spec = pl.BlockSpec((32, step, UNIT), lambda i: (0, i, 0))
    return pl.pallas_call(
        norm_back_kernel,
        grid=(tokens // step,),
        in_specs=[
            pl.BlockSpec(memory_space=pltpu.SMEM),
            unit_spec,
            unit_spec,
            pl.BlockSpec((step, width), lambda i: (i, 0)),
            pl.BlockSpec((step, UNIT), lambda i: (i, 0)),
            pl.BlockSpec((1, width), lambda i: (0, 0)),
        ],
        out_specs=pl.BlockSpec((step, width), lambda i: (i, 0)),
        out_shape=jax.ShapeDtypeStruct((tokens, width), BF16),
        name="norm_back",
    )(core, own, recv, source, inv, gain)


def grad_weight_kernel(place_ref, *refs):
    columns, grads, left, right = refs[:4], refs[4:12], refs[12:14], refs[14:18]
    out_ref, gain_ref = refs[18:]
    rows_each = UNIT // 2
    grad = jnp.concatenate([g[...] for g in grads], axis=0)
    half = grad.shape[1] // 2
    for i in range(4):
        at = [place_ref[2 * i + z] for z in (0, 1)]
        lhs = jnp.concatenate(
            [
                jnp.concatenate([c[t, at[0]], c[t, at[1]]], axis=1)
                for c in columns
                for t in (0, 1)
            ],
            axis=0,
        )
        part = lax.dot_general(lhs, grad, (((0,), (0,)), ((), ())), preferred_element_type=F32)
        weight = (
            left[i // 2][(i % 2) * 2 * UNIT : (i % 2 + 1) * 2 * UNIT, :],
            right[i][: 2 * UNIT, :],
        )
        dots = jnp.zeros((2 * UNIT, UNIT), F32)
        for side in (0, 1):
            both = part[:, side * half : (side + 1) * half] * weight[side].astype(F32)
            for col in range(0, half, UNIT):
                dots += both[:, col : col + UNIT]
        for z in (0, 1):
            turned = dots[z * UNIT : (z + 1) * UNIT].T
            gain_ref[pl.ds(at[z], 1), :] = jnp.sum(turned, axis=0, keepdims=True)
            for h in (0, 1):
                top = z * UNIT + h * rows_each
                out_ref[2 * at[z] + h, :rows_each, :] = part[top : top + rows_each].astype(BF16)
    rest = jnp.concatenate([gain_ref[u : u + 1, :] for u in range(8)], axis=1)
    terms = []
    for _ in range(3):
        terms.append(rest.astype(BF16).astype(F32))
        rest = rest - terms[-1]
    terms = jnp.concatenate(terms + [jnp.zeros((5, rest.shape[1]), F32)], axis=0).astype(BF16)
    for block in range(out_ref.shape[0]):
        out_ref[block, rows_each:, :] = terms


def grad_weight_part(place, columns, grads, left, right):
    units, width = columns[0].shape[1], grads[0].shape[1]
    whole = pl.BlockSpec(memory_space=pltpu.VMEM)
    return pl.pallas_call(
        grad_weight_kernel,
        in_specs=[pl.BlockSpec(memory_space=pltpu.SMEM)] + [whole] * 18,
        out_specs=whole,
        out_shape=jax.ShapeDtypeStruct((2 * units, UNIT // 2 + 8, width), BF16),
        scratch_shapes=[pltpu.VMEM((units, UNIT), F32)],
        compiler_params=pltpu.CompilerParams(vmem_limit_bytes=VMEM_LIMIT),
        name="grad_weight",
    )(place, *columns, *grads, *left, *right)


def gather_gain(total):
    other = shift(total, "core", 1)
    pair = jnp.where(
        lax.axis_index("core") == 0, jnp.stack([total, other]), jnp.stack([other, total])
    )
    found = [pair] + [shift(pair, "x", by) for by in range(1, 4)]
    x = lax.axis_index("x")
    in_order = []
    for at in range(4):
        piece = found[0]
        for by in range(1, 4):
            piece = jnp.where((x - by) % 4 == at, found[by], piece)
        in_order.append(piece)
    both = jnp.stack(in_order).reshape(4, 2, 8, UNIT)
    return both.transpose(2, 1, 0, 3).reshape(-1)


def step(layer_input, queries, grad_out, segment_ids, kv_weight, norm_gain):
    source = layer_input[0]
    tokens = source.shape[0]
    core = lax.axis_index("core").astype(jnp.int32)[None]
    x = lax.axis_index("x").astype(jnp.int32)[None]
    gain = norm_gain[None]
    table = unit_table()
    zs, ys = lax.axis_index("zlo"), lax.axis_index("y")
    turn = jnp.arange(8, dtype=jnp.int32)
    rel = jnp.repeat(jnp.array(REL4, jnp.int32), 2)
    unit_place = ((zs + turn) % 2 * 4 + (ys + rel) % 4).astype(jnp.int32)

    doc = (segment_ids + 1).astype(F32)
    doc_rows = jnp.broadcast_to(doc, (8, tokens))

    near, far = gather_weight(kv_weight)
    own, send, inv = normalize(core, source, gain)
    other = shift(send, "core", 1)
    blocks = spread(x, own, other)

    kv_near = project_near(table, own, other, near)
    kv_mine, kv_theirs = project_far(table, own, other, kv_near, far)
    kv_own = finish(kv_mine, shift(kv_theirs, "core", 1), doc_rows)

    kv_blocks = [kv_own] + [shift_seq(kv_own, k) for k in range(1, BACK + 1)]
    columns = [shift(block, "x", by) if by else block for by, block in enumerate(blocks)]
    attended, grad_queries, grad_here, *grad_back = attention(
        doc, queries[0], grad_out[0], kv_blocks
    )
    total = grad_here
    for k, part in enumerate(grad_back):
        total = total + shift_seq(part, -(k + 1)).astype(F32)
    grad_own = total.astype(BF16)
    grad_other = shift(grad_own, "core", 1)
    grads = [grad_own, grad_other]
    fars = [shift(grad_own, "x", by) for by in range(1, 4)]
    for block in fars:
        grads += [block, shift(block, "core", 1)]

    mine, theirs = grad_normed(table, grad_own, grad_other, near + far)
    left_own, right_own = near[:2], [near[6], near[8], near[10], far[2]]
    partial = grad_weight_part(unit_place, columns, grads, left_own, right_own)
    arrived = lax.all_to_all(partial, ("zlo", "y", "zhi"), 0, 0, tiled=True)
    arrived = jnp.sum(arrived.astype(F32), axis=0)
    grad_weight = arrived[: kv_weight.shape[0]]
    sums = arrived[kv_weight.shape[0] :]
    grad_gain = gather_gain(sums[0] + sums[1] + sums[2]) / norm_gain
    theirs = shift(theirs, "core", 1)
    grad_input = norm_back(core, mine, theirs, source, inv, gain)
    return attended[None], grad_queries[None], grad_input[None], grad_weight, grad_gain


def solution(mesh):
    fine = Mesh(mesh.devices.reshape(tuple(SIZES.values())), tuple(SIZES))
    tokens = P(BLK, SEQ, None)
    weight = P(BLK + SEQ, None)
    return jax.shard_map(
        step,
        mesh=fine,
        in_specs=(tokens, tokens, tokens, P(BLK, SEQ), weight, P()),
        out_specs=(tokens, tokens, tokens, weight, P()),
        check_vma=False,
    )
```

```python
import functools

import jax
import jax.numpy as jnp
from jax import lax
from jax.experimental import pallas as pl
from jax.experimental.pallas import tpu as pltpu
from jax.sharding import Mesh, PartitionSpec as P


HEAD = 128
UNIT = 128
BACK = 4
EPSILON = 1e-05
BF16 = jnp.bfloat16
F32 = jnp.float32
VMEM_LIMIT = 56 * 1024 * 1024

SIZES = {"zlo": 2, "y": 4, "core": 2, "x": 4, "zhi": 2}
BLK = ("zlo", "y", "core")
SEQ = ("x", "zhi")
REL4 = (0, -1, 1, 2)


def shift(value, axis, by):
    n = SIZES[axis]
    return lax.ppermute(value, axis, [(i, (i + by) % n) for i in range(n)])


def shift_seq(value, by):
    n = SIZES["x"] * SIZES["zhi"]
    pairs = [(i, i + by) for i in range(n) if 0 <= i + by < n]
    return lax.ppermute(value, SEQ, pairs)


def rows(pieces):
    return jnp.concatenate(pieces, axis=0)


def ring4(value, axis):
    half = value.shape[0] // 2
    before = shift(value, axis, 1)
    after = shift(value, axis, -1)
    far = [shift(before[:half], axis, 1), shift(after[half:], axis, -1)]
    first = join([value, before])
    second = join([after] + far)
    return first, second


def ring4_halves(first, second, axis):
    before_first, after_first = shift(first, axis, 1), shift(first, axis, -1)
    before_second, after_second = shift(second, axis, 1), shift(second, axis, -1)
    far_first = shift(before_first, axis, 1)
    far_second = shift(after_second, axis, -1)
    near = [first, second, before_first, after_first]
    return near, [before_second, after_second], [far_first, far_second]


def join_kernel(*refs):
    out_ref, at = refs[-1], 0
    for piece in refs[:-1]:
        out_ref[at : at + piece.shape[0], :] = piece[...]
        at += piece.shape[0]


def join(pieces):
    whole = pl.BlockSpec(memory_space=pltpu.VMEM)
    size = sum(piece.shape[0] for piece in pieces)
    return pl.pallas_call(
        join_kernel,
        in_specs=[whole] * len(pieces),
        out_specs=whole,
        out_shape=jax.ShapeDtypeStruct((size, pieces[0].shape[1]), BF16),
        name="join",
    )(*pieces)


def gather_weight(weight):
    other = shift(weight, "zhi", 1)
    across = shift(weight, "zlo", 1)
    both = lax.ppermute(weight, ("zlo", "zhi"), [(i, 3 - i) for i in range(4)])
    pair = jnp.where(
        lax.axis_index("zhi") == 0,
        rows([weight, other, across, both]),
        rows([other, weight, both, across]),
    )
    half = pair.shape[1] // 2
    left = ring4(pair[:, :half], "y")
    right = ring4(pair[:, half:], "x")
    lots = zip(ring4_halves(*left, "x"), ring4_halves(*right, "y"))
    return [at_left + at_right for at_left, at_right in lots]


def unit_table():
    zlo, y, x = lax.axis_index("zlo"), lax.axis_index("y"), lax.axis_index("x")
    rel = jnp.array(REL4, jnp.int32)
    zs = (zlo + jnp.arange(2, dtype=jnp.int32)) % 2
    ys, xs = (y + rel) % 4, (x + rel) % 4
    left = xs[:, None, None] * 8 + zs[None, None, :] * 4 + ys[None, :, None]
    right = xs[None, :, None] * 8 + zs[None, None, :] * 4 + ys[:, None, None]
    return jnp.stack([left, right]).reshape(64).astype(jnp.int32)


NEAR = tuple((side, side * 32 + first) for side in (0, 1) for first in (0, 4, 8, 16))
MORE = tuple((side, side * 32 + first) for side in (0, 1) for first in (12, 20))
FAR = tuple((side, side * 32 + first) for side in (0, 1) for first in (24, 28))
COUNT = 4


def norm_kernel(core_ref, x_ref, gain_ref, own_ref, send_ref, inv_ref):
    source = x_ref[...].astype(F32)
    inv = lax.rsqrt(jnp.mean(source * source, axis=1, keepdims=True) + EPSILON)
    inv_ref[...] = jnp.broadcast_to(inv, inv_ref.shape)
    first = core_ref[0] == 0
    for u in range(32):
        lo = ((u % 8) * 8 + u // 8) * UNIT
        hi = lo + 4 * UNIT
        parts = []
        for at in (lo, hi):
            part = x_ref[:, at : at + UNIT].astype(F32) * inv * gain_ref[:, at : at + UNIT]
            parts.append(part.astype(BF16))
        own_ref[u] = jnp.where(first, parts[0], parts[1])
        send_ref[u] = jnp.where(first, parts[1], parts[0])


def normalize(core, source, gain):
    tokens, width = source.shape
    step = 32
    return pl.pallas_call(
        norm_kernel,
        grid=(tokens // step,),
        in_specs=[
            pl.BlockSpec(memory_space=pltpu.SMEM),
            pl.BlockSpec((step, width), lambda i: (i, 0)),
            pl.BlockSpec((1, width), lambda i: (0, 0)),
        ],
        out_specs=[
            pl.BlockSpec((32, step, UNIT), lambda i: (0, i, 0)),
            pl.BlockSpec((32, step, UNIT), lambda i: (0, i, 0)),
            pl.BlockSpec((step, UNIT), lambda i: (i, 0)),
        ],
        out_shape=[
            jax.ShapeDtypeStruct((32, tokens, UNIT), BF16),
            jax.ShapeDtypeStruct((32, tokens, UNIT), BF16),
            jax.ShapeDtypeStruct((tokens, UNIT), F32),
        ],
        name="norm",
    )(core, source, gain)


def spread_kernel(x_ref, own_ref, other_ref, *outs):
    for by, out in enumerate(outs):
        at = lax.rem(x_ref[0] + by, 4) * 8
        out[0] = own_ref[pl.ds(at, 8)]
        out[1] = other_ref[pl.ds(at, 8)]


def spread(x, own, other):
    tokens = own.shape[1]
    whole = pl.BlockSpec(memory_space=pltpu.VMEM)
    return pl.pallas_call(
        spread_kernel,
        in_specs=[pl.BlockSpec(memory_space=pltpu.SMEM), whole, whole],
        out_specs=[whole] * 4,
        out_shape=[jax.ShapeDtypeStruct((2, 8, tokens, UNIT), BF16)] * 4,
        name="spread",
    )(x, own, other)


def project_sum(table_ref, own_ref, other_ref, pieces, refs, side):
    total = None
    for (at_side, first), piece in zip(pieces, refs):
        if at_side != side:
            continue
        top = [own_ref[table_ref[first + j]] for j in range(COUNT)]
        low = [other_ref[table_ref[first + j]] for j in range(COUNT)]
        lhs = jnp.concatenate(
            [jnp.concatenate(top, axis=1), jnp.concatenate(low, axis=1)], axis=0
        )
        term = jnp.dot(lhs, piece[...], preferred_element_type=F32)
        total = term if total is None else total + term
    return total


def project_lot_kernel(table_ref, own_ref, other_ref, *refs, lot):
    pieces, out_ref = refs[: len(lot)], refs[-1]
    for side in (0, 1):
        total = project_sum(table_ref, own_ref, other_ref, lot, pieces, side)
        width = total.shape[1]
        cols = slice(side * width, (side + 1) * width)
        if len(refs) > len(lot) + 1:
            total = total + refs[len(lot)][:, cols]
        out_ref[:, cols] = total


def project_lot(table, own, other, lot, pieces, *before):
    tokens = own.shape[1]
    width = 2 * pieces[0].shape[1]
    whole = pl.BlockSpec(memory_space=pltpu.VMEM)
    return pl.pallas_call(
        functools.partial(project_lot_kernel, lot=lot),
        in_specs=[pl.BlockSpec(memory_space=pltpu.SMEM)]
        + [whole] * (2 + len(pieces) + len(before)),
        out_specs=whole,
        out_shape=jax.ShapeDtypeStruct((2 * tokens, width), F32),
        compiler_params=pltpu.CompilerParams(vmem_limit_bytes=VMEM_LIMIT),
        name="project_lot",
    )(table, own, other, *pieces, *before)


def project_far_kernel(table_ref, own_ref, other_ref, near_ref, *refs):
    pieces, (mine_ref, theirs_ref) = refs[:-2], refs[-2:]
    tokens = own_ref.shape[1]
    for side in (0, 1):
        total = project_sum(table_ref, own_ref, other_ref, FAR, pieces, side)
        width = total.shape[1]
        cols = slice(side * width, (side + 1) * width)
        total = total + near_ref[:, cols]
        mine_ref[:, cols] = total[:tokens]
        theirs_ref[:, cols] = total[tokens:]


def project_far(table, own, other, near, pieces):
    tokens = own.shape[1]
    whole = pl.BlockSpec(memory_space=pltpu.VMEM)
    return pl.pallas_call(
        project_far_kernel,
        in_specs=[pl.BlockSpec(memory_space=pltpu.SMEM)] + [whole] * (3 + len(pieces)),
        out_specs=[whole, whole],
        out_shape=[jax.ShapeDtypeStruct((tokens, near.shape[1]), F32)] * 2,
        compiler_params=pltpu.CompilerParams(vmem_limit_bytes=VMEM_LIMIT),
        name="project_far",
    )(table, own, other, near, *pieces)


def finish_kernel(mine_ref, other_ref, doc_ref, out_ref):
    tokens = mine_ref.shape[0]
    out_ref[:tokens, :] = (mine_ref[...] + other_ref[...]).astype(BF16)
    out_ref[tokens:, :] = jnp.zeros((8, out_ref.shape[1]), BF16)
    out_ref[tokens:, :tokens] = doc_ref[...].astype(BF16)


def finish(mine, other, doc_rows):
    tokens, width = mine.shape
    whole = pl.BlockSpec(memory_space=pltpu.VMEM)
    return pl.pallas_call(
        finish_kernel,
        in_specs=[whole] * 3,
        out_specs=whole,
        out_shape=jax.ShapeDtypeStruct((tokens + 8, width), BF16),
        name="finish",
    )(mine, other, doc_rows)


def attention_kernel(doc_ref, q_ref, go_ref, *refs):
    keys, values = refs[: BACK + 1], refs[BACK + 1 : 2 * BACK + 2]
    docs, refs = refs[2 * BACK + 2 : 3 * BACK + 3], refs[3 * BACK + 3 :]
    att_ref, dq_ref, own_ref = refs[:3]
    back_refs = refs[3 : BACK + 3]
    probs_ref, grads_ref, q_rows, go_rows, bias_ref = refs[BACK + 3 : BACK + 8]
    score_ref, expo_ref, half_ref, gp_ref = refs[BACK + 8 :]
    head = pl.program_id(0)
    scale = HEAD ** (-0.5)
    group = q_ref.shape[1] // HEAD
    tokens = q_ref.shape[0]

    @pl.when(head == 0)
    def _():
        shape = (tokens, tokens)
        later = lax.broadcasted_iota(jnp.int32, shape, 0) > lax.broadcasted_iota(
            jnp.int32, shape, 1
        )
        for k, ref in enumerate(docs):
            of_key = jnp.broadcast_to(ref[:1, :].astype(F32), shape).T
            bias = jnp.where(of_key == doc_ref[...], 0.0, -1e30)
            bias_ref[k * tokens : (k + 1) * tokens, :] = (
                bias if k else jnp.where(later, -1e30, bias)
            )

    key = jnp.concatenate([r[...] for r in keys], axis=0)
    value = jnp.concatenate([r[...] for r in values], axis=0)
    key_t = key.astype(F32).T.astype(BF16)
    value_t = value.astype(F32).T.astype(BF16)
    nt = (((1,), (1,)), ((), ()))
    blocks = [slice(k * tokens, (k + 1) * tokens) for k in range(BACK + 1)]

    def fold(block, op):
        return op(block.reshape(tokens // 8, 8, tokens), axis=0)

    def products(j):
        cols = slice(j * HEAD, (j + 1) * HEAD)
        q, go = q_ref[:, cols], go_ref[:, cols]
        q_rows[j * tokens : (j + 1) * tokens, :] = q
        go_rows[j * tokens : (j + 1) * tokens, :] = go
        score_ref[j % 2] = lax.dot_general(key, q, nt, preferred_element_type=F32)
        gp_ref[j % 3] = lax.dot_general(value, go, nt, preferred_element_type=F32)

    def soften(j):
        cols = slice(j * HEAD, (j + 1) * HEAD)
        top = None
        for at in blocks:
            score = score_ref[j % 2, at] * scale + bias_ref[at]
            score_ref[j % 2, at] = score
            part = fold(score, jnp.max)
            top = part if top is None else jnp.maximum(top, part)
        top = jnp.max(top, axis=0, keepdims=True)
        total = jnp.zeros((8, tokens), F32)
        for at in blocks:
            expo = jnp.exp(score_ref[j % 2, at] - top)
            expo_ref[j % 2, at] = expo
            half_ref[j % 2, at] = expo.astype(BF16)
            total = total + fold(expo, jnp.sum)
        total = jnp.sum(total, axis=0, keepdims=True)
        summed = jnp.dot(value_t, half_ref[j % 2], preferred_element_type=F32) / total
        att = summed.astype(BF16).astype(F32)
        delta = jnp.sum(att * go_ref[:, cols].astype(F32).T, axis=0, keepdims=True)
        att_ref[:, cols] = att.T.astype(BF16)
        return 1.0 / total, delta

    def gradients(j, inverse, delta):
        cols = slice(j * HEAD, (j + 1) * HEAD)
        for at in blocks:
            probs = expo_ref[j % 2, at] * inverse
            probs_ref[at, cols] = probs.astype(BF16)
            grads_ref[at, cols] = (probs * (gp_ref[j % 3, at] - delta)).astype(BF16)
        dq = jnp.dot(key_t, grads_ref[:, cols], preferred_element_type=F32) * scale
        dq_ref[:, cols] = dq.T.astype(BF16)

    products(0)
    products(1)
    rows_of = soften(0)
    for j in range(group):
        if j + 2 < group:
            products(j + 2)
        following = soften(j + 1) if j + 1 < group else None
        gradients(j, *rows_of)
        rows_of = following
    grad_key = jnp.dot(grads_ref[...], q_rows[...], preferred_element_type=F32) * scale
    grad_value = jnp.dot(probs_ref[...], go_rows[...], preferred_element_type=F32)
    kv_width = own_ref.shape[1] // 2
    key_at = pl.multiple_of(head * HEAD, HEAD)
    value_at = pl.multiple_of(kv_width + head * HEAD, HEAD)
    own_ref[:, pl.ds(key_at, HEAD)] = grad_key[:tokens]
    own_ref[:, pl.ds(value_at, HEAD)] = grad_value[:tokens]
    for k, ref in enumerate(back_refs):
        at = slice((k + 1) * tokens, (k + 2) * tokens)
        ref[:, pl.ds(key_at, HEAD)] = grad_key[at].astype(BF16)
        ref[:, pl.ds(value_at, HEAD)] = grad_value[at].astype(BF16)


def attention(doc, queries, grad_out, kv_blocks):
    tokens, q_width = queries.shape
    kv_total = kv_blocks[0].shape[1]
    kv_heads = kv_total // 2 // HEAD
    group_cols = q_width // kv_heads
    span = (BACK + 1) * tokens
    q_spec = pl.BlockSpec((tokens, group_cols), lambda h: (0, h))
    key_spec = pl.BlockSpec((tokens, HEAD), lambda h: (0, h))
    value_spec = pl.BlockSpec((tokens, HEAD), lambda h: (0, kv_heads + h))
    doc_spec = pl.BlockSpec((8, tokens), lambda h: (tokens // 8, 0))
    grad_spec = pl.BlockSpec((tokens, kv_total), lambda h: (0, 0))
    return pl.pallas_call(
        attention_kernel,
        grid=(kv_heads,),
        in_specs=[pl.BlockSpec((1, tokens), lambda h: (0, 0)), q_spec, q_spec]
        + [key_spec] * (BACK + 1)
        + [value_spec] * (BACK + 1)
        + [doc_spec] * (BACK + 1),
        out_specs=[q_spec, q_spec] + [grad_spec] * (BACK + 1),
        out_shape=[
            jax.ShapeDtypeStruct((tokens, q_width), BF16),
            jax.ShapeDtypeStruct((tokens, q_width), BF16),
            jax.ShapeDtypeStruct((tokens, kv_total), F32),
        ]
        + [jax.ShapeDtypeStruct((tokens, kv_total), BF16)] * BACK,
        scratch_shapes=[
            pltpu.VMEM((span, group_cols), BF16),
            pltpu.VMEM((span, group_cols), BF16),
            pltpu.VMEM((tokens * group_cols // HEAD, HEAD), BF16),
            pltpu.VMEM((tokens * group_cols // HEAD, HEAD), BF16),
            pltpu.VMEM((span, tokens), F32),
            pltpu.VMEM((2, span, tokens), F32),
            pltpu.VMEM((2, span, tokens), F32),
            pltpu.VMEM((2, span, tokens), BF16),
            pltpu.VMEM((3, span, tokens), F32),
        ],
        compiler_params=pltpu.CompilerParams(vmem_limit_bytes=VMEM_LIMIT),
        name="attention",
    )(doc, queries, grad_out, *kv_blocks, *kv_blocks, *kv_blocks)


def grad_normed_kernel(table_ref, mine_ref, theirs_ref, *refs):
    pieces, (own_ref, send_ref, acc_ref) = refs[:-3], refs[-3:]
    tokens = mine_ref.shape[0]
    nt = (((1,), (1,)), ((), ()))
    order = sorted(zip(NEAR + MORE + FAR, pieces), key=lambda entry: entry[0])
    for (side, first), piece in order:
        width = piece.shape[1]
        cols = slice(side * width, (side + 1) * width)
        lhs = jnp.concatenate([mine_ref[:, cols], theirs_ref[:, cols]], axis=0)
        term = lax.dot_general(lhs, piece[...], nt, preferred_element_type=F32)
        for j in range(COUNT):
            u = table_ref[first + j]
            part = term[:, j * UNIT : (j + 1) * UNIT]
            if side == 0:
                acc_ref[u] = part
            else:
                part = (part + acc_ref[u]).astype(BF16)
                own_ref[u] = part[:tokens]
                send_ref[u] = part[tokens:]


def grad_normed(table, mine, theirs, pieces):
    tokens = mine.shape[0]
    whole = pl.BlockSpec(memory_space=pltpu.VMEM)
    return pl.pallas_call(
        grad_normed_kernel,
        in_specs=[pl.BlockSpec(memory_space=pltpu.SMEM)] + [whole] * (2 + len(pieces)),
        out_specs=[whole, whole],
        out_shape=[jax.ShapeDtypeStruct((32, tokens, UNIT), BF16)] * 2,
        scratch_shapes=[pltpu.VMEM((32, 2 * tokens, UNIT), F32)],
        compiler_params=pltpu.CompilerParams(vmem_limit_bytes=VMEM_LIMIT),
        name="grad_normed",
    )(table, mine, theirs, *pieces)


def norm_back_kernel(core_ref, own_ref, recv_ref, x_ref, inv_ref, gain_ref, out_ref):
    first = core_ref[0] == 0
    inv = inv_ref[:, :1]
    width = x_ref.shape[1]
    step = x_ref.shape[0]

    def unit(at):
        u = (at % 4) * 8 + at // 8
        same = first if (at % 8) < 4 else jnp.logical_not(first)
        cols = slice(at * UNIT, (at + 1) * UNIT)
        grad = jnp.where(same, own_ref[u], recv_ref[u]).astype(F32)
        scaled = x_ref[:, cols].astype(F32) * inv
        return cols, grad, scaled

    dots = jnp.zeros((step, UNIT), F32)
    for at in range(width // UNIT):
        cols, grad, scaled = unit(at)
        dots += grad * gain_ref[:, cols] * scaled
    mean = jnp.sum(dots, axis=1, keepdims=True) * (1.0 / width)
    for at in range(width // UNIT):
        cols, grad, scaled = unit(at)
        out_ref[:, cols] = (inv * (grad * gain_ref[:, cols] - scaled * mean)).astype(BF16)


def norm_back(core, own, recv, source, inv, gain):
    tokens, width = source.shape
    step = 32
    unit_spec = pl.BlockSpec((32, step, UNIT), lambda i: (0, i, 0))
    return pl.pallas_call(
        norm_back_kernel,
        grid=(tokens // step,),
        in_specs=[
            pl.BlockSpec(memory_space=pltpu.SMEM),
            unit_spec,
            unit_spec,
            pl.BlockSpec((step, width), lambda i: (i, 0)),
            pl.BlockSpec((step, UNIT), lambda i: (i, 0)),
            pl.BlockSpec((1, width), lambda i: (0, 0)),
        ],
        out_specs=pl.BlockSpec((step, width), lambda i: (i, 0)),
        out_shape=jax.ShapeDtypeStruct((tokens, width), BF16),
        name="norm_back",
    )(core, own, recv, source, inv, gain)


def grad_weight_kernel(place_ref, *refs):
    columns, grads, left, right = refs[:4], refs[4:12], refs[12:14], refs[14:18]
    first_ref, second_ref, gain_ref = refs[18:]
    rows_each, cut = UNIT // 2, UNIT // 4
    grad = jnp.concatenate([g[...] for g in grads], axis=0)
    half = grad.shape[1] // 2
    for i in range(4):
        at = [place_ref[2 * i + z] for z in (0, 1)]
        lhs = jnp.concatenate(
            [
                jnp.concatenate([c[t, at[0]], c[t, at[1]]], axis=1)
                for c in columns
                for t in (0, 1)
            ],
            axis=0,
        )
        part = lax.dot_general(lhs, grad, (((0,), (0,)), ((), ())), preferred_element_type=F32)
        weight = (
            left[i // 2][(i % 2) * 2 * UNIT : (i % 2 + 1) * 2 * UNIT, :],
            right[i][: 2 * UNIT, :],
        )
        dots = jnp.zeros((2 * UNIT, UNIT), F32)
        for side in (0, 1):
            both = part[:, side * half : (side + 1) * half] * weight[side].astype(F32)
            for col in range(0, half, UNIT):
                dots += both[:, col : col + UNIT]
        for z in (0, 1):
            turned = dots[z * UNIT : (z + 1) * UNIT].T
            gain_ref[pl.ds(at[z], 1), :] = jnp.sum(turned, axis=0, keepdims=True)
            for h in (0, 1):
                top = z * UNIT + h * rows_each
                block = part[top : top + rows_each].astype(BF16)
                first_ref[2 * at[z] + h, :cut, :] = block[:cut]
                second_ref[2 * at[z] + h] = block[cut:]
    rest = jnp.concatenate([gain_ref[u : u + 1, :] for u in range(8)], axis=1)
    terms = []
    for _ in range(3):
        terms.append(rest.astype(BF16).astype(F32))
        rest = rest - terms[-1]
    terms = jnp.concatenate(terms + [jnp.zeros((5, rest.shape[1]), F32)], axis=0).astype(BF16)
    for i in range(first_ref.shape[0]):
        first_ref[i, cut:, :] = terms


def grad_weight_part(place, columns, grads, left, right):
    units, width = columns[0].shape[1], grads[0].shape[1]
    whole = pl.BlockSpec(memory_space=pltpu.VMEM)
    return pl.pallas_call(
        grad_weight_kernel,
        in_specs=[pl.BlockSpec(memory_space=pltpu.SMEM)] + [whole] * 18,
        out_specs=[whole] * 2,
        out_shape=[
            jax.ShapeDtypeStruct((2 * units, UNIT // 4 + 8, width), BF16),
            jax.ShapeDtypeStruct((2 * units, UNIT // 4, width), BF16),
        ],
        scratch_shapes=[pltpu.VMEM((units, UNIT), F32)],
        compiler_params=pltpu.CompilerParams(vmem_limit_bytes=VMEM_LIMIT),
        name="grad_weight",
    )(place, *columns, *grads, *left, *right)


def gather_gain(total):
    other = shift(total, "core", 1)
    pair = jnp.where(
        lax.axis_index("core") == 0, jnp.stack([total, other]), jnp.stack([other, total])
    )
    found = [pair] + [shift(pair, "x", by) for by in range(1, 4)]
    x = lax.axis_index("x")
    in_order = []
    for at in range(4):
        piece = found[0]
        for by in range(1, 4):
            piece = jnp.where((x - by) % 4 == at, found[by], piece)
        in_order.append(piece)
    both = jnp.stack(in_order).reshape(4, 2, 8, UNIT)
    return both.transpose(2, 1, 0, 3).reshape(-1)


def step(layer_input, queries, grad_out, segment_ids, kv_weight, norm_gain):
    source = layer_input[0]
    tokens = source.shape[0]
    core = lax.axis_index("core").astype(jnp.int32)[None]
    x = lax.axis_index("x").astype(jnp.int32)[None]
    gain = norm_gain[None]
    table = unit_table()
    zs, ys = lax.axis_index("zlo"), lax.axis_index("y")
    turn = jnp.arange(8, dtype=jnp.int32)
    rel = jnp.repeat(jnp.array(REL4, jnp.int32), 2)
    unit_place = ((zs + turn) % 2 * 4 + (ys + rel) % 4).astype(jnp.int32)

    doc = (segment_ids + 1).astype(F32)
    doc_rows = jnp.broadcast_to(doc, (8, tokens))

    near, more, far = gather_weight(kv_weight)
    own, send, inv = normalize(core, source, gain)
    other = shift(send, "core", 1)
    blocks = spread(x, own, other)

    kv_near = project_lot(table, own, other, NEAR, near)
    kv_near = project_lot(table, own, other, MORE, more, kv_near)
    kv_mine, kv_theirs = project_far(table, own, other, kv_near, far)
    kv_own = finish(kv_mine, shift(kv_theirs, "core", 1), doc_rows)

    kv_blocks = [kv_own] + [shift_seq(kv_own, k) for k in range(1, BACK + 1)]
    columns = [shift(block, "x", by) if by else block for by, block in enumerate(blocks)]
    attended, grad_queries, grad_here, *grad_back = attention(
        doc, queries[0], grad_out[0], kv_blocks
    )
    total = grad_here
    for k, part in enumerate(grad_back):
        total = total + shift_seq(part, -(k + 1)).astype(F32)
    grad_own = total.astype(BF16)
    grad_other = shift(grad_own, "core", 1)
    grads = [grad_own, grad_other]
    fars = [shift(grad_own, "x", by) for by in range(1, 4)]
    for block in fars:
        grads += [block, shift(block, "core", 1)]

    mine, theirs = grad_normed(table, grad_own, grad_other, near + more + far)
    left_own, right_own = near[:2], [near[4], near[6], near[7], far[2]]
    halves = grad_weight_part(unit_place, columns, grads, left_own, right_own)
    group = ("zlo", "y", "zhi")
    arrived = lax.all_to_all(halves[0], group, 0, 0, tiled=True)
    arrived, later = lax.optimization_barrier((arrived, halves[1]))
    arrived = jnp.sum(arrived.astype(F32), axis=0)
    cut = kv_weight.shape[0] // 2
    sums = arrived[cut:]
    grad_gain = gather_gain(sums[0] + sums[1] + sums[2]) / norm_gain
    rest = lax.all_to_all(later, group, 0, 0, tiled=True)
    grad_weight = rows([arrived[:cut], jnp.sum(rest.astype(F32), axis=0)])
    theirs = shift(theirs, "core", 1)
    grad_input = norm_back(core, mine, theirs, source, inv, gain)
    return attended[None], grad_queries[None], grad_input[None], grad_weight, grad_gain


def solution(mesh):
    fine = Mesh(mesh.devices.reshape(tuple(SIZES.values())), tuple(SIZES))
    tokens = P(BLK, SEQ, None)
    weight = P(BLK + SEQ, None)
    return jax.shard_map(
        step,
        mesh=fine,
        in_specs=(tokens, tokens, tokens, P(BLK, SEQ), weight, P()),
        out_specs=(tokens, tokens, tokens, weight, P()),
        check_vma=False,
    )
```

```python
import functools

import jax
import jax.numpy as jnp
from jax import lax
from jax.experimental import pallas as pl
from jax.experimental.pallas import tpu as pltpu
from jax.sharding import Mesh, PartitionSpec as P


HEAD = 128
UNIT = 128
BACK = 4
EPSILON = 1e-05
BF16 = jnp.bfloat16
F32 = jnp.float32
VMEM_LIMIT = 56 * 1024 * 1024

SIZES = {"zlo": 2, "y": 4, "core": 2, "x": 4, "zhi": 2}
BLK = ("zlo", "y", "core")
SEQ = ("x", "zhi")
REL4 = (0, -1, 1, 2)


def shift(value, axis, by):
    n = SIZES[axis]
    return lax.ppermute(value, axis, [(i, (i + by) % n) for i in range(n)])


def shift_seq(value, by):
    n = SIZES["x"] * SIZES["zhi"]
    pairs = [(i, i + by) for i in range(n) if 0 <= i + by < n]
    return lax.ppermute(value, SEQ, pairs)


def in_vmem(arrays):
    return [pltpu.with_memory_space_constraint(a, pltpu.VMEM) for a in arrays]


def rows(pieces):
    return jnp.concatenate(pieces, axis=0)


def ring4(value, axis):
    before = shift(value, axis, 1)
    after = shift(value, axis, -1)
    far = shift(value, axis, 2)
    first = join([value, before])
    second = join([after, far])
    return first, second


def ring4_halves(first, second, axis):
    before_first, after_first = shift(first, axis, 1), shift(first, axis, -1)
    before_second, after_second = shift(second, axis, 1), shift(second, axis, -1)
    far_first = shift(before_first, axis, 1)
    far_second = shift(after_second, axis, -1)
    near = [first, second, before_first, after_first]
    return near, [before_second, after_second], [far_first, far_second]


def join_kernel(*refs):
    out_ref, at = refs[-1], 0
    for piece in refs[:-1]:
        out_ref[at : at + piece.shape[0], :] = piece[...]
        at += piece.shape[0]


def join(pieces):
    whole = pl.BlockSpec(memory_space=pltpu.VMEM)
    size = sum(piece.shape[0] for piece in pieces)
    return pl.pallas_call(
        join_kernel,
        in_specs=[whole] * len(pieces),
        out_specs=whole,
        out_shape=jax.ShapeDtypeStruct((size, pieces[0].shape[1]), BF16),
        name="join",
    )(*in_vmem(pieces))


def gather_weight(weight):
    other = shift(weight, "zhi", 1)
    across = shift(weight, "zlo", 1)
    both = lax.ppermute(weight, ("zlo", "zhi"), [(i, 3 - i) for i in range(4)])
    pair = jnp.where(
        lax.axis_index("zhi") == 0,
        rows([weight, other, across, both]),
        rows([other, weight, both, across]),
    )
    half = pair.shape[1] // 2
    left = ring4(pair[:, :half], "y")
    right = ring4(pair[:, half:], "x")
    lots = zip(ring4_halves(*left, "x"), ring4_halves(*right, "y"))
    return [at_left + at_right for at_left, at_right in lots]


def unit_table():
    zlo, y, x = lax.axis_index("zlo"), lax.axis_index("y"), lax.axis_index("x")
    rel = jnp.array(REL4, jnp.int32)
    zs = (zlo + jnp.arange(2, dtype=jnp.int32)) % 2
    ys, xs = (y + rel) % 4, (x + rel) % 4
    left = xs[:, None, None] * 8 + zs[None, None, :] * 4 + ys[None, :, None]
    right = xs[None, :, None] * 8 + zs[None, None, :] * 4 + ys[:, None, None]
    return jnp.stack([left, right]).reshape(64).astype(jnp.int32)


NEAR = tuple((side, side * 32 + first) for side in (0, 1) for first in (0, 4, 8, 16))
MORE = tuple((side, side * 32 + first) for side in (0, 1) for first in (12, 20))
FAR = tuple((side, side * 32 + first) for side in (0, 1) for first in (24, 28))
COUNT = 4


def norm_kernel(core_ref, x_ref, gain_ref, own_ref, send_ref, inv_ref):
    source = x_ref[...].astype(F32)
    inv = lax.rsqrt(jnp.mean(source * source, axis=1, keepdims=True) + EPSILON)
    inv_ref[...] = jnp.broadcast_to(inv, inv_ref.shape)
    first = core_ref[0] == 0
    for u in range(32):
        lo = ((u % 8) * 8 + u // 8) * UNIT
        hi = lo + 4 * UNIT
        parts = []
        for at in (lo, hi):
            part = x_ref[:, at : at + UNIT].astype(F32) * inv * gain_ref[:, at : at + UNIT]
            parts.append(part.astype(BF16))
        own_ref[u] = jnp.where(first, parts[0], parts[1])
        send_ref[u] = jnp.where(first, parts[1], parts[0])


def normalize(core, source, gain):
    tokens, width = source.shape
    step = 32
    return pl.pallas_call(
        norm_kernel,
        grid=(tokens // step,),
        in_specs=[
            pl.BlockSpec(memory_space=pltpu.SMEM),
            pl.BlockSpec((step, width), lambda i: (i, 0)),
            pl.BlockSpec((1, width), lambda i: (0, 0)),
        ],
        out_specs=[
            pl.BlockSpec((32, step, UNIT), lambda i: (0, i, 0)),
            pl.BlockSpec((32, step, UNIT), lambda i: (0, i, 0)),
            pl.BlockSpec((step, UNIT), lambda i: (i, 0)),
        ],
        out_shape=[
            jax.ShapeDtypeStruct((32, tokens, UNIT), BF16),
            jax.ShapeDtypeStruct((32, tokens, UNIT), BF16),
            jax.ShapeDtypeStruct((tokens, UNIT), F32),
        ],
        name="norm",
    )(core, source, gain)


def spread_kernel(x_ref, own_ref, other_ref, *outs):
    for by, out in enumerate(outs):
        at = lax.rem(x_ref[0] + by, 4) * 8
        out[0] = own_ref[pl.ds(at, 8)]
        out[1] = other_ref[pl.ds(at, 8)]


def spread(x, own, other):
    tokens = own.shape[1]
    whole = pl.BlockSpec(memory_space=pltpu.VMEM)
    return pl.pallas_call(
        spread_kernel,
        in_specs=[pl.BlockSpec(memory_space=pltpu.SMEM), whole, whole],
        out_specs=[whole] * 4,
        out_shape=[jax.ShapeDtypeStruct((2, 8, tokens, UNIT), BF16)] * 4,
        name="spread",
    )(x, own, other)


def project_sum(table_ref, own_ref, other_ref, pieces, refs, side):
    total = None
    for (at_side, first), piece in zip(pieces, refs):
        if at_side != side:
            continue
        top = [own_ref[table_ref[first + j]] for j in range(COUNT)]
        low = [other_ref[table_ref[first + j]] for j in range(COUNT)]
        lhs = jnp.concatenate(
            [jnp.concatenate(top, axis=1), jnp.concatenate(low, axis=1)], axis=0
        )
        term = jnp.dot(lhs, piece[...], preferred_element_type=F32)
        total = term if total is None else total + term
    return total


def project_lot_kernel(table_ref, own_ref, other_ref, *refs, lot):
    pieces, out_ref = refs[: len(lot)], refs[-1]
    for side in (0, 1):
        total = project_sum(table_ref, own_ref, other_ref, lot, pieces, side)
        width = total.shape[1]
        cols = slice(side * width, (side + 1) * width)
        if len(refs) > len(lot) + 1:
            total = total + refs[len(lot)][:, cols]
        out_ref[:, cols] = total


def project_lot(table, own, other, lot, pieces, *before):
    tokens = own.shape[1]
    width = 2 * pieces[0].shape[1]
    whole = pl.BlockSpec(memory_space=pltpu.VMEM)
    return pl.pallas_call(
        functools.partial(project_lot_kernel, lot=lot),
        in_specs=[pl.BlockSpec(memory_space=pltpu.SMEM)]
        + [whole] * (2 + len(pieces) + len(before)),
        out_specs=whole,
        out_shape=jax.ShapeDtypeStruct((2 * tokens, width), F32),
        compiler_params=pltpu.CompilerParams(vmem_limit_bytes=VMEM_LIMIT),
        name="project_lot",
    )(table, *in_vmem((own, other, *pieces, *before)))


def project_far_kernel(table_ref, own_ref, other_ref, near_ref, *refs):
    pieces, (mine_ref, theirs_ref) = refs[:-2], refs[-2:]
    tokens = own_ref.shape[1]
    for side in (0, 1):
        total = project_sum(table_ref, own_ref, other_ref, FAR, pieces, side)
        width = total.shape[1]
        cols = slice(side * width, (side + 1) * width)
        total = total + near_ref[:, cols]
        mine_ref[:, cols] = total[:tokens]
        theirs_ref[:, cols] = total[tokens:]


def project_far(table, own, other, near, pieces):
    tokens = own.shape[1]
    whole = pl.BlockSpec(memory_space=pltpu.VMEM)
    return pl.pallas_call(
        project_far_kernel,
        in_specs=[pl.BlockSpec(memory_space=pltpu.SMEM)] + [whole] * (3 + len(pieces)),
        out_specs=[whole, whole],
        out_shape=[jax.ShapeDtypeStruct((tokens, near.shape[1]), F32)] * 2,
        compiler_params=pltpu.CompilerParams(vmem_limit_bytes=VMEM_LIMIT),
        name="project_far",
    )(table, *in_vmem((own, other, near, *pieces)))


def finish_kernel(mine_ref, other_ref, doc_ref, out_ref):
    tokens = mine_ref.shape[0]
    out_ref[:tokens, :] = (mine_ref[...] + other_ref[...]).astype(BF16)
    out_ref[tokens:, :] = jnp.zeros((8, out_ref.shape[1]), BF16)
    out_ref[tokens:, :tokens] = jnp.broadcast_to(doc_ref[...], (8, tokens)).astype(BF16)


def finish(mine, other, doc):
    tokens, width = mine.shape
    whole = pl.BlockSpec(memory_space=pltpu.VMEM)
    return pl.pallas_call(
        finish_kernel,
        in_specs=[whole] * 3,
        out_specs=whole,
        out_shape=jax.ShapeDtypeStruct((tokens + 8, width), BF16),
        name="finish",
    )(*in_vmem([mine, other]), doc)


def attention_kernel(doc_ref, q_ref, go_ref, *refs):
    keys, values = refs[: BACK + 1], refs[BACK + 1 : 2 * BACK + 2]
    docs, refs = refs[2 * BACK + 2 : 3 * BACK + 3], refs[3 * BACK + 3 :]
    att_ref, dq_ref, own_ref = refs[:3]
    back_refs = refs[3 : BACK + 3]
    probs_ref, grads_ref, q_rows, go_rows, bias_ref = refs[BACK + 3 : BACK + 8]
    score_ref, expo_ref, half_ref, gp_ref = refs[BACK + 8 :]
    head = pl.program_id(0)
    scale = HEAD ** (-0.5)
    group = q_ref.shape[1] // HEAD
    tokens = q_ref.shape[0]

    @pl.when(head == 0)
    def _():
        shape = (tokens, tokens)
        later = lax.broadcasted_iota(jnp.int32, shape, 0) > lax.broadcasted_iota(
            jnp.int32, shape, 1
        )
        for k, ref in enumerate(docs):
            of_key = jnp.broadcast_to(ref[:1, :].astype(F32), shape).T
            bias = jnp.where(of_key == doc_ref[...], 0.0, -1e30)
            bias_ref[k * tokens : (k + 1) * tokens, :] = (
                bias if k else jnp.where(later, -1e30, bias)
            )

    key = jnp.concatenate([r[...] for r in keys], axis=0)
    value = jnp.concatenate([r[...] for r in values], axis=0)
    key_t = key.astype(F32).T.astype(BF16)
    value_t = value.astype(F32).T.astype(BF16)
    nt = (((1,), (1,)), ((), ()))
    blocks = [slice(k * tokens, (k + 1) * tokens) for k in range(BACK + 1)]

    def fold(block, op):
        return op(block.reshape(tokens // 8, 8, tokens), axis=0)

    def products(j):
        cols = slice(j * HEAD, (j + 1) * HEAD)
        q, go = q_ref[:, cols], go_ref[:, cols]
        q_rows[j * tokens : (j + 1) * tokens, :] = q
        go_rows[j * tokens : (j + 1) * tokens, :] = go
        score_ref[j % 2] = lax.dot_general(key, q, nt, preferred_element_type=F32)
        gp_ref[j % 3] = lax.dot_general(value, go, nt, preferred_element_type=F32)

    def soften(j):
        cols = slice(j * HEAD, (j + 1) * HEAD)
        top = None
        for at in blocks:
            score = score_ref[j % 2, at] * scale + bias_ref[at]
            score_ref[j % 2, at] = score
            part = fold(score, jnp.max)
            top = part if top is None else jnp.maximum(top, part)
        top = jnp.max(top, axis=0, keepdims=True)
        total = jnp.zeros((8, tokens), F32)
        for at in blocks:
            expo = jnp.exp(score_ref[j % 2, at] - top)
            expo_ref[j % 2, at] = expo
            half_ref[j % 2, at] = expo.astype(BF16)
            total = total + fold(expo, jnp.sum)
        total = jnp.sum(total, axis=0, keepdims=True)
        summed = jnp.dot(value_t, half_ref[j % 2], preferred_element_type=F32) / total
        att = summed.astype(BF16).astype(F32)
        delta = jnp.sum(att * go_ref[:, cols].astype(F32).T, axis=0, keepdims=True)
        att_ref[:, cols] = att.T.astype(BF16)
        return 1.0 / total, delta

    def gradients(j, inverse, delta):
        cols = slice(j * HEAD, (j + 1) * HEAD)
        for at in blocks:
            probs = expo_ref[j % 2, at] * inverse
            probs_ref[at, cols] = probs.astype(BF16)
            grads_ref[at, cols] = (probs * (gp_ref[j % 3, at] - delta)).astype(BF16)
        dq = jnp.dot(key_t, grads_ref[:, cols], preferred_element_type=F32) * scale
        dq_ref[:, cols] = dq.T.astype(BF16)

    products(0)
    products(1)
    rows_of = soften(0)
    for j in range(group):
        if j + 2 < group:
            products(j + 2)
        following = soften(j + 1) if j + 1 < group else None
        gradients(j, *rows_of)
        rows_of = following
    grad_key = jnp.dot(grads_ref[...], q_rows[...], preferred_element_type=F32) * scale
    grad_value = jnp.dot(probs_ref[...], go_rows[...], preferred_element_type=F32)
    kv_width = own_ref.shape[1] // 2
    key_at = pl.multiple_of(head * HEAD, HEAD)
    value_at = pl.multiple_of(kv_width + head * HEAD, HEAD)
    own_ref[:, pl.ds(key_at, HEAD)] = grad_key[:tokens]
    own_ref[:, pl.ds(value_at, HEAD)] = grad_value[:tokens]
    for k, ref in enumerate(back_refs):
        at = slice((k + 1) * tokens, (k + 2) * tokens)
        ref[:, pl.ds(key_at, HEAD)] = grad_key[at].astype(BF16)
        ref[:, pl.ds(value_at, HEAD)] = grad_value[at].astype(BF16)


def attention(doc, queries, grad_out, kv_blocks):
    tokens, q_width = queries.shape
    kv_total = kv_blocks[0].shape[1]
    kv_heads = kv_total // 2 // HEAD
    group_cols = q_width // kv_heads
    span = (BACK + 1) * tokens
    q_spec = pl.BlockSpec((tokens, group_cols), lambda h: (0, h))
    key_spec = pl.BlockSpec((tokens, HEAD), lambda h: (0, h))
    value_spec = pl.BlockSpec((tokens, HEAD), lambda h: (0, kv_heads + h))
    doc_spec = pl.BlockSpec((8, tokens), lambda h: (tokens // 8, 0))
    grad_spec = pl.BlockSpec((tokens, kv_total), lambda h: (0, 0))
    return pl.pallas_call(
        attention_kernel,
        grid=(kv_heads,),
        in_specs=[pl.BlockSpec((1, tokens), lambda h: (0, 0)), q_spec, q_spec]
        + [key_spec] * (BACK + 1)
        + [value_spec] * (BACK + 1)
        + [doc_spec] * (BACK + 1),
        out_specs=[q_spec, q_spec] + [grad_spec] * (BACK + 1),
        out_shape=[
            jax.ShapeDtypeStruct((tokens, q_width), BF16),
            jax.ShapeDtypeStruct((tokens, q_width), BF16),
            jax.ShapeDtypeStruct((tokens, kv_total), F32),
        ]
        + [jax.ShapeDtypeStruct((tokens, kv_total), BF16)] * BACK,
        scratch_shapes=[
            pltpu.VMEM((span, group_cols), BF16),
            pltpu.VMEM((span, group_cols), BF16),
            pltpu.VMEM((tokens * group_cols // HEAD, HEAD), BF16),
            pltpu.VMEM((tokens * group_cols // HEAD, HEAD), BF16),
            pltpu.VMEM((span, tokens), F32),
            pltpu.VMEM((2, span, tokens), F32),
            pltpu.VMEM((2, span, tokens), F32),
            pltpu.VMEM((2, span, tokens), BF16),
            pltpu.VMEM((3, span, tokens), F32),
        ],
        compiler_params=pltpu.CompilerParams(vmem_limit_bytes=VMEM_LIMIT),
        name="attention",
    )(doc, queries, grad_out, *kv_blocks, *kv_blocks, *kv_blocks)


def grad_normed_kernel(table_ref, mine_ref, theirs_ref, *refs):
    pieces, (own_ref, send_ref, acc_ref) = refs[:-3], refs[-3:]
    tokens = mine_ref.shape[0]
    nt = (((1,), (1,)), ((), ()))
    order = sorted(zip(NEAR + MORE + FAR, pieces), key=lambda entry: entry[0])
    for (side, first), piece in order:
        width = piece.shape[1]
        cols = slice(side * width, (side + 1) * width)
        lhs = jnp.concatenate([mine_ref[:, cols], theirs_ref[:, cols]], axis=0)
        term = lax.dot_general(lhs, piece[...], nt, preferred_element_type=F32)
        for j in range(COUNT):
            u = table_ref[first + j]
            part = term[:, j * UNIT : (j + 1) * UNIT]
            if side == 0:
                acc_ref[u] = part
            else:
                part = (part + acc_ref[u]).astype(BF16)
                own_ref[u] = part[:tokens]
                send_ref[u] = part[tokens:]


def grad_normed(table, mine, theirs, pieces):
    tokens = mine.shape[0]
    whole = pl.BlockSpec(memory_space=pltpu.VMEM)
    return pl.pallas_call(
        grad_normed_kernel,
        in_specs=[pl.BlockSpec(memory_space=pltpu.SMEM)] + [whole] * (2 + len(pieces)),
        out_specs=[whole, whole],
        out_shape=[jax.ShapeDtypeStruct((32, tokens, UNIT), BF16)] * 2,
        scratch_shapes=[pltpu.VMEM((32, 2 * tokens, UNIT), F32)],
        compiler_params=pltpu.CompilerParams(vmem_limit_bytes=VMEM_LIMIT),
        name="grad_normed",
    )(table, mine, theirs, *pieces)


def norm_back_kernel(core_ref, own_ref, recv_ref, x_ref, inv_ref, gain_ref, out_ref):
    first = core_ref[0] == 0
    inv = inv_ref[:, :1]
    width = x_ref.shape[1]
    step = x_ref.shape[0]

    def unit(at):
        u = (at % 4) * 8 + at // 8
        same = first if (at % 8) < 4 else jnp.logical_not(first)
        cols = slice(at * UNIT, (at + 1) * UNIT)
        grad = jnp.where(same, own_ref[u], recv_ref[u]).astype(F32)
        scaled = x_ref[:, cols].astype(F32) * inv
        return cols, grad, scaled

    dots = jnp.zeros((step, UNIT), F32)
    for at in range(width // UNIT):
        cols, grad, scaled = unit(at)
        dots += grad * gain_ref[:, cols] * scaled
    mean = jnp.sum(dots, axis=1, keepdims=True) * (1.0 / width)
    for at in range(width // UNIT):
        cols, grad, scaled = unit(at)
        out_ref[:, cols] = (inv * (grad * gain_ref[:, cols] - scaled * mean)).astype(BF16)


def norm_back(core, own, recv, source, inv, gain):
    tokens, width = source.shape
    step = 32
    unit_spec = pl.BlockSpec((32, step, UNIT), lambda i: (0, i, 0))
    return pl.pallas_call(
        norm_back_kernel,
        grid=(tokens // step,),
        in_specs=[
            pl.BlockSpec(memory_space=pltpu.SMEM),
            unit_spec,
            unit_spec,
            pl.BlockSpec((step, width), lambda i: (i, 0)),
            pl.BlockSpec((step, UNIT), lambda i: (i, 0)),
            pl.BlockSpec((1, width), lambda i: (0, 0)),
        ],
        out_specs=pl.BlockSpec((step, width), lambda i: (i, 0)),
        out_shape=jax.ShapeDtypeStruct((tokens, width), BF16),
        name="norm_back",
    )(core, own, recv, source, inv, gain)


def grad_weight_kernel(place_ref, *refs):
    columns, grads, left, right = refs[:4], refs[4:12], refs[12:14], refs[14:18]
    first_ref, second_ref, gain_ref = refs[18:]
    rows_each, cut = UNIT // 2, UNIT // 4
    grad = jnp.concatenate([g[...] for g in grads], axis=0)
    half = grad.shape[1] // 2
    for i in range(4):
        at = [place_ref[2 * i + z] for z in (0, 1)]
        lhs = jnp.concatenate(
            [
                jnp.concatenate([c[t, at[0]], c[t, at[1]]], axis=1)
                for c in columns
                for t in (0, 1)
            ],
            axis=0,
        )
        part = lax.dot_general(lhs, grad, (((0,), (0,)), ((), ())), preferred_element_type=F32)
        weight = (
            left[i // 2][(i % 2) * 2 * UNIT : (i % 2 + 1) * 2 * UNIT, :],
            right[i][: 2 * UNIT, :],
        )
        dots = jnp.zeros((2 * UNIT, UNIT), F32)
        for side in (0, 1):
            both = part[:, side * half : (side + 1) * half] * weight[side].astype(F32)
            for col in range(0, half, UNIT):
                dots += both[:, col : col + UNIT]
        for z in (0, 1):
            turned = dots[z * UNIT : (z + 1) * UNIT].T
            gain_ref[pl.ds(at[z], 1), :] = jnp.sum(turned, axis=0, keepdims=True)
            for h in (0, 1):
                top = z * UNIT + h * rows_each
                block = part[top : top + rows_each].astype(BF16)
                first_ref[2 * at[z] + h, :cut, :] = block[:cut]
                second_ref[2 * at[z] + h] = block[cut:]
    rest = jnp.concatenate([gain_ref[u : u + 1, :] for u in range(8)], axis=1)
    terms = []
    for _ in range(3):
        terms.append(rest.astype(BF16).astype(F32))
        rest = rest - terms[-1]
    terms = jnp.concatenate(terms + [jnp.zeros((5, rest.shape[1]), F32)], axis=0).astype(BF16)
    for i in range(first_ref.shape[0]):
        first_ref[i, cut:, :] = terms


def grad_weight_part(place, columns, grads, left, right):
    units, width = columns[0].shape[1], grads[0].shape[1]
    whole = pl.BlockSpec(memory_space=pltpu.VMEM)
    return pl.pallas_call(
        grad_weight_kernel,
        in_specs=[pl.BlockSpec(memory_space=pltpu.SMEM)] + [whole] * 18,
        out_specs=[whole] * 2,
        out_shape=[
            jax.ShapeDtypeStruct((2 * units, UNIT // 4 + 8, width), BF16),
            jax.ShapeDtypeStruct((2 * units, UNIT // 4, width), BF16),
        ],
        scratch_shapes=[pltpu.VMEM((units, UNIT), F32)],
        compiler_params=pltpu.CompilerParams(vmem_limit_bytes=VMEM_LIMIT),
        name="grad_weight",
    )(place, *columns, *in_vmem(grads), *left, *right)


def gather_gain(total):
    other = shift(total, "core", 1)
    pair = jnp.where(
        lax.axis_index("core") == 0, jnp.stack([total, other]), jnp.stack([other, total])
    )
    found = [pair] + [shift(pair, "x", by) for by in range(1, 4)]
    x = lax.axis_index("x")
    in_order = []
    for at in range(4):
        piece = found[0]
        for by in range(1, 4):
            piece = jnp.where((x - by) % 4 == at, found[by], piece)
        in_order.append(piece)
    both = jnp.stack(in_order).reshape(4, 2, 8, UNIT)
    return both.transpose(2, 1, 0, 3).reshape(-1)


def step(layer_input, queries, grad_out, segment_ids, kv_weight, norm_gain):
    source = layer_input[0]
    core = lax.axis_index("core").astype(jnp.int32)[None]
    x = lax.axis_index("x").astype(jnp.int32)[None]
    gain = norm_gain[None]
    table = unit_table()
    zs, ys = lax.axis_index("zlo"), lax.axis_index("y")
    turn = jnp.arange(8, dtype=jnp.int32)
    rel = jnp.repeat(jnp.array(REL4, jnp.int32), 2)
    unit_place = ((zs + turn) % 2 * 4 + (ys + rel) % 4).astype(jnp.int32)

    doc = (segment_ids + 1).astype(F32)
    near, more, far = gather_weight(kv_weight)
    own, send, inv = normalize(core, source, gain)
    other = shift(send, "core", 1)
    blocks = spread(x, own, other)

    kv_near = project_lot(table, own, other, NEAR, near)
    kv_near = project_lot(table, own, other, MORE, more, kv_near)
    kv_mine, kv_theirs = project_far(table, own, other, kv_near, far)
    kv_own = finish(kv_mine, shift(kv_theirs, "core", 1), doc)

    kv_blocks = [kv_own] + [shift_seq(kv_own, k) for k in range(1, BACK + 1)]
    columns = [shift(block, "x", by) if by else block for by, block in enumerate(blocks)]
    attended, grad_queries, grad_here, *grad_back = attention(
        doc, queries[0], grad_out[0], kv_blocks
    )
    total = grad_here
    for k, part in enumerate(grad_back):
        total = total + shift_seq(part, -(k + 1)).astype(F32)
    grad_own = total.astype(BF16)
    grad_other = shift(grad_own, "core", 1)
    grads = [grad_own, grad_other]
    fars = [shift(grad_own, "x", by) for by in range(1, 4)]
    for block in fars:
        grads += [block, shift(block, "core", 1)]

    mine, theirs = grad_normed(table, grad_own, grad_other, near + more + far)
    left_own, right_own = near[:2], [near[4], near[6], near[7], far[2]]
    halves = grad_weight_part(unit_place, columns, grads, left_own, right_own)
    group = ("zlo", "y", "zhi")
    arrived = lax.all_to_all(halves[0], group, 0, 0, tiled=True)
    arrived, later = lax.optimization_barrier((arrived, halves[1]))
    arrived = jnp.sum(arrived.astype(F32), axis=0)
    cut = kv_weight.shape[0] // 2
    sums = arrived[cut:]
    grad_gain = gather_gain(sums[0] + sums[1] + sums[2]) / norm_gain
    rest = lax.all_to_all(later, group, 0, 0, tiled=True)
    grad_weight = rows([arrived[:cut], jnp.sum(rest.astype(F32), axis=0)])
    theirs = shift(theirs, "core", 1)
    grad_input = norm_back(core, mine, theirs, source, inv, gain)
    return attended[None], grad_queries[None], grad_input[None], grad_weight, grad_gain


def solution(mesh):
    fine = Mesh(mesh.devices.reshape(tuple(SIZES.values())), tuple(SIZES))
    tokens = P(BLK, SEQ, None)
    weight = P(BLK + SEQ, None)
    return jax.shard_map(
        step,
        mesh=fine,
        in_specs=(tokens, tokens, tokens, P(BLK, SEQ), weight, P()),
        out_specs=(tokens, tokens, tokens, weight, P()),
        check_vma=False,
    )
```

```python
import functools

import jax
import jax.numpy as jnp
from jax import lax
from jax.experimental import pallas as pl
from jax.experimental.pallas import tpu as pltpu
from jax.sharding import Mesh, PartitionSpec as P


HEAD = 128
UNIT = 128
BACK = 4
EPSILON = 1e-05
BF16 = jnp.bfloat16
F32 = jnp.float32
VMEM_LIMIT = 56 * 1024 * 1024

SIZES = {"zlo": 2, "y": 4, "core": 2, "x": 4, "zhi": 2}
BLK = ("zlo", "y", "core")
SEQ = ("x", "zhi")
REL4 = (0, -1, 1, 2)


def shift(value, axis, by):
    n = SIZES[axis]
    return lax.ppermute(value, axis, [(i, (i + by) % n) for i in range(n)])


def shift_seq(value, by):
    n = SIZES["x"] * SIZES["zhi"]
    pairs = [(i, i + by) for i in range(n) if 0 <= i + by < n]
    return lax.ppermute(value, SEQ, pairs)


def in_vmem(arrays):
    return [pltpu.with_memory_space_constraint(a, pltpu.VMEM) for a in arrays]


def rows(pieces):
    return jnp.concatenate(pieces, axis=0)


def ring4(value, axis):
    before = shift(value, axis, 1)
    after = shift(value, axis, -1)
    far = shift(value, axis, 2)
    first = join([value, before])
    second = join([after, far])
    return first, second


def ring4_halves(first, second, axis):
    before_first, after_first = shift(first, axis, 1), shift(first, axis, -1)
    before_second, after_second = shift(second, axis, 1), shift(second, axis, -1)
    far_first = shift(before_first, axis, 1)
    far_second = shift(after_second, axis, -1)
    near = [first, second, before_first, after_first]
    return near, [before_second, after_second], [far_first, far_second]


def join_kernel(*refs):
    out_ref, at = refs[-1], 0
    for piece in refs[:-1]:
        out_ref[at : at + piece.shape[0], :] = piece[...]
        at += piece.shape[0]


def join(pieces):
    whole = pl.BlockSpec(memory_space=pltpu.VMEM)
    size = sum(piece.shape[0] for piece in pieces)
    return pl.pallas_call(
        join_kernel,
        in_specs=[whole] * len(pieces),
        out_specs=whole,
        out_shape=jax.ShapeDtypeStruct((size, pieces[0].shape[1]), BF16),
        name="join",
    )(*in_vmem(pieces))


def gather_weight(weight):
    other = shift(weight, "zhi", 1)
    across = shift(weight, "zlo", 1)
    both = lax.ppermute(weight, ("zlo", "zhi"), [(i, 3 - i) for i in range(4)])
    pair = jnp.where(
        lax.axis_index("zhi") == 0,
        rows([weight, other, across, both]),
        rows([other, weight, both, across]),
    )
    half = pair.shape[1] // 2
    left = ring4(pair[:, :half], "y")
    right = ring4(pair[:, half:], "x")
    lots = zip(ring4_halves(*left, "x"), ring4_halves(*right, "y"))
    return [at_left + at_right for at_left, at_right in lots]


def unit_table():
    zlo, y, x = lax.axis_index("zlo"), lax.axis_index("y"), lax.axis_index("x")
    rel = jnp.array(REL4, jnp.int32)
    zs = (zlo + jnp.arange(2, dtype=jnp.int32)) % 2
    ys, xs = (y + rel) % 4, (x + rel) % 4
    left = xs[:, None, None] * 8 + zs[None, None, :] * 4 + ys[None, :, None]
    right = xs[None, :, None] * 8 + zs[None, None, :] * 4 + ys[:, None, None]
    return jnp.stack([left, right]).reshape(64).astype(jnp.int32)


NEAR = tuple((side, side * 32 + first) for side in (0, 1) for first in (0, 4, 8, 16))
MORE = tuple((side, side * 32 + first) for side in (0, 1) for first in (12, 20))
FAR = tuple((side, side * 32 + first) for side in (0, 1) for first in (24, 28))
COUNT = 4


def norm_kernel(core_ref, x_ref, gain_ref, own_ref, send_ref, inv_ref):
    source = x_ref[...].astype(F32)
    inv = lax.rsqrt(jnp.mean(source * source, axis=1, keepdims=True) + EPSILON)
    inv_ref[...] = jnp.broadcast_to(inv, inv_ref.shape)
    first = core_ref[0] == 0
    for u in range(32):
        lo = ((u % 8) * 8 + u // 8) * UNIT
        hi = lo + 4 * UNIT
        parts = []
        for at in (lo, hi):
            part = x_ref[:, at : at + UNIT].astype(F32) * inv * gain_ref[:, at : at + UNIT]
            parts.append(part.astype(BF16))
        own_ref[u] = jnp.where(first, parts[0], parts[1])
        send_ref[u] = jnp.where(first, parts[1], parts[0])


def normalize(core, source, gain):
    tokens, width = source.shape
    step = 32
    return pl.pallas_call(
        norm_kernel,
        grid=(tokens // step,),
        in_specs=[
            pl.BlockSpec(memory_space=pltpu.SMEM),
            pl.BlockSpec((step, width), lambda i: (i, 0)),
            pl.BlockSpec((1, width), lambda i: (0, 0)),
        ],
        out_specs=[
            pl.BlockSpec((32, step, UNIT), lambda i: (0, i, 0)),
            pl.BlockSpec((32, step, UNIT), lambda i: (0, i, 0)),
            pl.BlockSpec((step, UNIT), lambda i: (i, 0)),
        ],
        out_shape=[
            jax.ShapeDtypeStruct((32, tokens, UNIT), BF16),
            jax.ShapeDtypeStruct((32, tokens, UNIT), BF16),
            jax.ShapeDtypeStruct((tokens, UNIT), F32),
        ],
        name="norm",
    )(core, source, gain)


def spread_kernel(x_ref, own_ref, other_ref, *outs):
    for by, out in enumerate(outs):
        at = lax.rem(x_ref[0] + by, 4) * 8
        out[0] = own_ref[pl.ds(at, 8)]
        out[1] = other_ref[pl.ds(at, 8)]


def spread(x, own, other):
    tokens = own.shape[1]
    whole = pl.BlockSpec(memory_space=pltpu.VMEM)
    return pl.pallas_call(
        spread_kernel,
        in_specs=[pl.BlockSpec(memory_space=pltpu.SMEM), whole, whole],
        out_specs=[whole] * 4,
        out_shape=[jax.ShapeDtypeStruct((2, 8, tokens, UNIT), BF16)] * 4,
        name="spread",
    )(x, own, other)


def project_sum(table_ref, own_ref, other_ref, pieces, refs, side):
    total = None
    for (at_side, first), piece in zip(pieces, refs):
        if at_side != side:
            continue
        top = [own_ref[table_ref[first + j]] for j in range(COUNT)]
        low = [other_ref[table_ref[first + j]] for j in range(COUNT)]
        lhs = jnp.concatenate(
            [jnp.concatenate(top, axis=1), jnp.concatenate(low, axis=1)], axis=0
        )
        term = jnp.dot(lhs, piece[...], preferred_element_type=F32)
        total = term if total is None else total + term
    return total


def project_lot_kernel(table_ref, own_ref, other_ref, *refs, lot):
    pieces, out_ref = refs[: len(lot)], refs[-1]
    for side in (0, 1):
        total = project_sum(table_ref, own_ref, other_ref, lot, pieces, side)
        width = total.shape[1]
        cols = slice(side * width, (side + 1) * width)
        if len(refs) > len(lot) + 1:
            total = total + refs[len(lot)][:, cols]
        out_ref[:, cols] = total


def project_lot(table, own, other, lot, pieces, *before):
    tokens = own.shape[1]
    width = 2 * pieces[0].shape[1]
    whole = pl.BlockSpec(memory_space=pltpu.VMEM)
    return pl.pallas_call(
        functools.partial(project_lot_kernel, lot=lot),
        in_specs=[pl.BlockSpec(memory_space=pltpu.SMEM)]
        + [whole] * (2 + len(pieces) + len(before)),
        out_specs=whole,
        out_shape=jax.ShapeDtypeStruct((2 * tokens, width), F32),
        compiler_params=pltpu.CompilerParams(vmem_limit_bytes=VMEM_LIMIT),
        name="project_lot",
    )(table, *in_vmem((own, other, *pieces, *before)))


def project_far_kernel(table_ref, own_ref, other_ref, near_ref, *refs):
    pieces, (mine_ref, theirs_ref) = refs[:-2], refs[-2:]
    tokens = own_ref.shape[1]
    for side in (0, 1):
        total = project_sum(table_ref, own_ref, other_ref, FAR, pieces, side)
        width = total.shape[1]
        cols = slice(side * width, (side + 1) * width)
        total = total + near_ref[:, cols]
        mine_ref[:, cols] = total[:tokens]
        theirs_ref[:, cols] = total[tokens:]


def project_far(table, own, other, near, pieces):
    tokens = own.shape[1]
    whole = pl.BlockSpec(memory_space=pltpu.VMEM)
    return pl.pallas_call(
        project_far_kernel,
        in_specs=[pl.BlockSpec(memory_space=pltpu.SMEM)] + [whole] * (3 + len(pieces)),
        out_specs=[whole, whole],
        out_shape=[jax.ShapeDtypeStruct((tokens, near.shape[1]), F32)] * 2,
        compiler_params=pltpu.CompilerParams(vmem_limit_bytes=VMEM_LIMIT),
        name="project_far",
    )(table, *in_vmem((own, other, near, *pieces)))


def finish_kernel(mine_ref, other_ref, doc_ref, out_ref):
    tokens = mine_ref.shape[0]
    out_ref[:tokens, :] = (mine_ref[...] + other_ref[...]).astype(BF16)
    out_ref[tokens:, :] = jnp.zeros((8, out_ref.shape[1]), BF16)
    out_ref[tokens:, :tokens] = jnp.broadcast_to(doc_ref[...], (8, tokens)).astype(BF16)


def finish(mine, other, doc):
    tokens, width = mine.shape
    whole = pl.BlockSpec(memory_space=pltpu.VMEM)
    return pl.pallas_call(
        finish_kernel,
        in_specs=[whole] * 3,
        out_specs=whole,
        out_shape=jax.ShapeDtypeStruct((tokens + 8, width), BF16),
        name="finish",
    )(*in_vmem([mine, other]), doc)


def attention_kernel(doc_ref, q_ref, go_ref, *refs):
    keys, values = refs[: BACK + 1], refs[BACK + 1 : 2 * BACK + 2]
    docs, refs = refs[2 * BACK + 2 : 3 * BACK + 3], refs[3 * BACK + 3 :]
    att_ref, dq_ref, own_ref = refs[:3]
    back_refs = refs[3 : BACK + 3]
    probs_ref, grads_ref, q_rows, go_rows, bias_ref = refs[BACK + 3 : BACK + 8]
    score_ref, expo_ref, half_ref, gp_ref = refs[BACK + 8 :]
    head = pl.program_id(0)
    scale = HEAD ** (-0.5)
    group = q_ref.shape[1] // HEAD
    tokens = q_ref.shape[0]

    @pl.when(head == 0)
    def _():
        shape = (tokens, tokens)
        later = lax.broadcasted_iota(jnp.int32, shape, 0) > lax.broadcasted_iota(
            jnp.int32, shape, 1
        )
        for k, ref in enumerate(docs):
            of_key = jnp.broadcast_to(ref[:1, :].astype(F32), shape).T
            bias = jnp.where(of_key == doc_ref[...], 0.0, -1e30)
            bias_ref[k * tokens : (k + 1) * tokens, :] = (
                bias if k else jnp.where(later, -1e30, bias)
            )

    key = jnp.concatenate([r[...] for r in keys], axis=0)
    value = jnp.concatenate([r[...] for r in values], axis=0)
    key_t = key.astype(F32).T.astype(BF16)
    value_t = value.astype(F32).T.astype(BF16)
    nt = (((1,), (1,)), ((), ()))
    blocks = [slice(k * tokens, (k + 1) * tokens) for k in range(BACK + 1)]

    def fold(block, op):
        return op(block.reshape(tokens // 8, 8, tokens), axis=0)

    def products(j):
        cols = slice(j * HEAD, (j + 1) * HEAD)
        q, go = q_ref[:, cols], go_ref[:, cols]
        q_rows[j * tokens : (j + 1) * tokens, :] = q
        go_rows[j * tokens : (j + 1) * tokens, :] = go
        score_ref[j % 2] = lax.dot_general(key, q, nt, preferred_element_type=F32)
        gp_ref[j % 3] = lax.dot_general(value, go, nt, preferred_element_type=F32)

    def soften(j):
        cols = slice(j * HEAD, (j + 1) * HEAD)
        top = None
        for at in blocks:
            score = score_ref[j % 2, at] * scale + bias_ref[at]
            score_ref[j % 2, at] = score
            part = fold(score, jnp.max)
            top = part if top is None else jnp.maximum(top, part)
        top = jnp.max(top, axis=0, keepdims=True)
        total = jnp.zeros((8, tokens), F32)
        for at in blocks:
            expo = jnp.exp(score_ref[j % 2, at] - top)
            expo_ref[j % 2, at] = expo
            half_ref[j % 2, at] = expo.astype(BF16)
            total = total + fold(expo, jnp.sum)
        total = jnp.sum(total, axis=0, keepdims=True)
        summed = jnp.dot(value_t, half_ref[j % 2], preferred_element_type=F32) / total
        att = summed.astype(BF16).astype(F32)
        delta = jnp.sum(att * go_ref[:, cols].astype(F32).T, axis=0, keepdims=True)
        att_ref[:, cols] = att.T.astype(BF16)
        return 1.0 / total, delta

    def gradients(j, inverse, delta):
        cols = slice(j * HEAD, (j + 1) * HEAD)
        for at in blocks:
            probs = expo_ref[j % 2, at] * inverse
            probs_ref[at, cols] = probs.astype(BF16)
            grads_ref[at, cols] = (probs * (gp_ref[j % 3, at] - delta)).astype(BF16)
        dq = jnp.dot(key_t, grads_ref[:, cols], preferred_element_type=F32) * scale
        dq_ref[:, cols] = dq.T.astype(BF16)

    products(0)
    products(1)
    rows_of = soften(0)
    for j in range(group):
        if j + 2 < group:
            products(j + 2)
        following = soften(j + 1) if j + 1 < group else None
        gradients(j, *rows_of)
        rows_of = following
    grad_key = jnp.dot(grads_ref[...], q_rows[...], preferred_element_type=F32) * scale
    grad_value = jnp.dot(probs_ref[...], go_rows[...], preferred_element_type=F32)
    kv_width = own_ref.shape[1] // 2
    key_at = pl.multiple_of(head * HEAD, HEAD)
    value_at = pl.multiple_of(kv_width + head * HEAD, HEAD)
    own_ref[:, pl.ds(key_at, HEAD)] = grad_key[:tokens]
    own_ref[:, pl.ds(value_at, HEAD)] = grad_value[:tokens]
    for k, ref in enumerate(back_refs):
        at = slice((k + 1) * tokens, (k + 2) * tokens)
        ref[:, pl.ds(key_at, HEAD)] = grad_key[at].astype(BF16)
        ref[:, pl.ds(value_at, HEAD)] = grad_value[at].astype(BF16)


def attention(doc, queries, grad_out, kv_blocks):
    tokens, q_width = queries.shape
    kv_total = kv_blocks[0].shape[1]
    kv_heads = kv_total // 2 // HEAD
    group_cols = q_width // kv_heads
    span = (BACK + 1) * tokens
    q_spec = pl.BlockSpec((tokens, group_cols), lambda h: (0, h))
    key_spec = pl.BlockSpec((tokens, HEAD), lambda h: (0, h))
    value_spec = pl.BlockSpec((tokens, HEAD), lambda h: (0, kv_heads + h))
    doc_spec = pl.BlockSpec((8, tokens), lambda h: (tokens // 8, 0))
    grad_spec = pl.BlockSpec((tokens, kv_total), lambda h: (0, 0))
    return pl.pallas_call(
        attention_kernel,
        grid=(kv_heads,),
        in_specs=[pl.BlockSpec((1, tokens), lambda h: (0, 0)), q_spec, q_spec]
        + [key_spec] * (BACK + 1)
        + [value_spec] * (BACK + 1)
        + [doc_spec] * (BACK + 1),
        out_specs=[q_spec, q_spec] + [grad_spec] * (BACK + 1),
        out_shape=[
            jax.ShapeDtypeStruct((tokens, q_width), BF16),
            jax.ShapeDtypeStruct((tokens, q_width), BF16),
            jax.ShapeDtypeStruct((tokens, kv_total), F32),
        ]
        + [jax.ShapeDtypeStruct((tokens, kv_total), BF16)] * BACK,
        scratch_shapes=[
            pltpu.VMEM((span, group_cols), BF16),
            pltpu.VMEM((span, group_cols), BF16),
            pltpu.VMEM((tokens * group_cols // HEAD, HEAD), BF16),
            pltpu.VMEM((tokens * group_cols // HEAD, HEAD), BF16),
            pltpu.VMEM((span, tokens), F32),
            pltpu.VMEM((2, span, tokens), F32),
            pltpu.VMEM((2, span, tokens), F32),
            pltpu.VMEM((2, span, tokens), BF16),
            pltpu.VMEM((3, span, tokens), F32),
        ],
        compiler_params=pltpu.CompilerParams(vmem_limit_bytes=VMEM_LIMIT),
        name="attention",
    )(doc, queries, grad_out, *kv_blocks, *kv_blocks, *kv_blocks)


def grad_normed_kernel(table_ref, mine_ref, theirs_ref, *refs):
    pieces, (own_ref, send_ref, acc_ref) = refs[:-3], refs[-3:]
    tokens = mine_ref.shape[0]
    nt = (((1,), (1,)), ((), ()))
    order = sorted(zip(NEAR + MORE + FAR, pieces), key=lambda entry: entry[0])
    for (side, first), piece in order:
        width = piece.shape[1]
        cols = slice(side * width, (side + 1) * width)
        lhs = jnp.concatenate([mine_ref[:, cols], theirs_ref[:, cols]], axis=0)
        term = lax.dot_general(lhs, piece[...], nt, preferred_element_type=F32)
        for j in range(COUNT):
            u = table_ref[first + j]
            part = term[:, j * UNIT : (j + 1) * UNIT]
            if side == 0:
                acc_ref[u] = part
            else:
                part = (part + acc_ref[u]).astype(BF16)
                own_ref[u] = part[:tokens]
                send_ref[u] = part[tokens:]


def grad_normed(table, mine, theirs, pieces):
    tokens = mine.shape[0]
    whole = pl.BlockSpec(memory_space=pltpu.VMEM)
    return pl.pallas_call(
        grad_normed_kernel,
        in_specs=[pl.BlockSpec(memory_space=pltpu.SMEM)] + [whole] * (2 + len(pieces)),
        out_specs=[whole, whole],
        out_shape=[jax.ShapeDtypeStruct((32, tokens, UNIT), BF16)] * 2,
        scratch_shapes=[pltpu.VMEM((32, 2 * tokens, UNIT), F32)],
        compiler_params=pltpu.CompilerParams(vmem_limit_bytes=VMEM_LIMIT),
        name="grad_normed",
    )(table, mine, theirs, *pieces)


def norm_back_kernel(core_ref, own_ref, recv_ref, x_ref, inv_ref, gain_ref, out_ref):
    first = core_ref[0] == 0
    inv = inv_ref[:, :1]
    width = x_ref.shape[1]
    step = x_ref.shape[0]

    def unit(at):
        u = (at % 4) * 8 + at // 8
        same = first if (at % 8) < 4 else jnp.logical_not(first)
        cols = slice(at * UNIT, (at + 1) * UNIT)
        grad = jnp.where(same, own_ref[u], recv_ref[u]).astype(F32)
        scaled = x_ref[:, cols].astype(F32) * inv
        return cols, grad, scaled

    dots = jnp.zeros((step, UNIT), F32)
    for at in range(width // UNIT):
        cols, grad, scaled = unit(at)
        dots += grad * gain_ref[:, cols] * scaled
    mean = jnp.sum(dots, axis=1, keepdims=True) * (1.0 / width)
    for at in range(width // UNIT):
        cols, grad, scaled = unit(at)
        out_ref[:, cols] = (inv * (grad * gain_ref[:, cols] - scaled * mean)).astype(BF16)


def norm_back(core, own, recv, source, inv, gain):
    tokens, width = source.shape
    step = 32
    unit_spec = pl.BlockSpec((32, step, UNIT), lambda i: (0, i, 0))
    return pl.pallas_call(
        norm_back_kernel,
        grid=(tokens // step,),
        in_specs=[
            pl.BlockSpec(memory_space=pltpu.SMEM),
            unit_spec,
            unit_spec,
            pl.BlockSpec((step, width), lambda i: (i, 0)),
            pl.BlockSpec((step, UNIT), lambda i: (i, 0)),
            pl.BlockSpec((1, width), lambda i: (0, 0)),
        ],
        out_specs=pl.BlockSpec((step, width), lambda i: (i, 0)),
        out_shape=jax.ShapeDtypeStruct((tokens, width), BF16),
        name="norm_back",
    )(core, own, recv, source, inv, gain)


def grad_weight_kernel(place_ref, *refs):
    columns, grads, left, right = refs[:4], refs[4:12], refs[12:14], refs[14:18]
    first_ref, second_ref, gain_ref = refs[18:]
    rows_each, cut = UNIT // 2, UNIT // 4
    grad = jnp.concatenate([g[...] for g in grads], axis=0)
    half = grad.shape[1] // 2
    for i in range(4):
        at = [place_ref[2 * i + z] for z in (0, 1)]
        lhs = jnp.concatenate(
            [
                jnp.concatenate([c[t, at[0]], c[t, at[1]]], axis=1)
                for c in columns
                for t in (0, 1)
            ],
            axis=0,
        )
        part = lax.dot_general(lhs, grad, (((0,), (0,)), ((), ())), preferred_element_type=F32)
        weight = (
            left[i // 2][(i % 2) * 2 * UNIT : (i % 2 + 1) * 2 * UNIT, :],
            right[i][: 2 * UNIT, :],
        )
        dots = jnp.zeros((2 * UNIT, UNIT), F32)
        for side in (0, 1):
            both = part[:, side * half : (side + 1) * half] * weight[side].astype(F32)
            for col in range(0, half, UNIT):
                dots += both[:, col : col + UNIT]
        for z in (0, 1):
            turned = dots[z * UNIT : (z + 1) * UNIT].T
            gain_ref[pl.ds(at[z], 1), :] = jnp.sum(turned, axis=0, keepdims=True)
            for h in (0, 1):
                top = z * UNIT + h * rows_each
                block = part[top : top + rows_each].astype(BF16)
                first_ref[2 * at[z] + h, :cut, :] = block[:cut]
                second_ref[2 * at[z] + h] = block[cut:]
    rest = jnp.concatenate([gain_ref[u : u + 1, :] for u in range(8)], axis=1)
    terms = []
    for _ in range(3):
        terms.append(rest.astype(BF16).astype(F32))
        rest = rest - terms[-1]
    terms = jnp.concatenate(terms + [jnp.zeros((5, rest.shape[1]), F32)], axis=0).astype(BF16)
    for i in range(first_ref.shape[0]):
        first_ref[i, cut:, :] = terms


def grad_weight_part(place, columns, grads, left, right):
    units, width = columns[0].shape[1], grads[0].shape[1]
    whole = pl.BlockSpec(memory_space=pltpu.VMEM)
    return pl.pallas_call(
        grad_weight_kernel,
        in_specs=[pl.BlockSpec(memory_space=pltpu.SMEM)] + [whole] * 18,
        out_specs=[whole] * 2,
        out_shape=[
            jax.ShapeDtypeStruct((2 * units, UNIT // 4 + 8, width), BF16),
            jax.ShapeDtypeStruct((2 * units, UNIT // 4, width), BF16),
        ],
        scratch_shapes=[pltpu.VMEM((units, UNIT), F32)],
        compiler_params=pltpu.CompilerParams(vmem_limit_bytes=VMEM_LIMIT),
        name="grad_weight",
    )(place, *columns, *in_vmem(grads), *left, *right)


def gather_gain(total):
    other = shift(total, "core", 1)
    pair = jnp.where(
        lax.axis_index("core") == 0, jnp.stack([total, other]), jnp.stack([other, total])
    )
    found = [pair] + [shift(pair, "x", by) for by in range(1, 4)]
    x = lax.axis_index("x")
    in_order = []
    for at in range(4):
        piece = found[0]
        for by in range(1, 4):
            piece = jnp.where((x - by) % 4 == at, found[by], piece)
        in_order.append(piece)
    both = jnp.stack(in_order).reshape(4, 2, 8, UNIT)
    return both.transpose(2, 1, 0, 3).reshape(-1)


def step(layer_input, queries, grad_out, segment_ids, kv_weight, norm_gain):
    source = layer_input[0]
    core = lax.axis_index("core").astype(jnp.int32)[None]
    x = lax.axis_index("x").astype(jnp.int32)[None]
    gain = norm_gain[None]
    table = unit_table()
    zs, ys = lax.axis_index("zlo"), lax.axis_index("y")
    turn = jnp.arange(8, dtype=jnp.int32)
    rel = jnp.repeat(jnp.array(REL4, jnp.int32), 2)
    unit_place = ((zs + turn) % 2 * 4 + (ys + rel) % 4).astype(jnp.int32)

    doc = (segment_ids + 1).astype(F32)
    near, more, far = gather_weight(kv_weight)
    own, send, inv = normalize(core, source, gain)
    other = shift(send, "core", 1)
    blocks = spread(x, own, other)

    kv_near = project_lot(table, own, other, NEAR, near)
    kv_near = project_lot(table, own, other, MORE, more, kv_near)
    kv_mine, kv_theirs = project_far(table, own, other, kv_near, far)
    kv_own = finish(kv_mine, shift(kv_theirs, "core", 1), doc)

    distant = [shift_seq(kv_own, k) for k in (3, 4)]
    kv_blocks = [kv_own] + [shift_seq(kv_own, k) for k in (1, 2)] + distant
    columns = [shift(block, "x", by) if by else block for by, block in enumerate(blocks)]
    attended, grad_queries, grad_here, *grad_back = attention(
        doc, queries[0], grad_out[0], kv_blocks
    )
    total = grad_here
    for k, part in enumerate(grad_back):
        total = total + shift_seq(part, -(k + 1)).astype(F32)
    grad_own = total.astype(BF16)
    grad_other = shift(grad_own, "core", 1)
    grads = [grad_own, grad_other]
    opposite = shift(grad_own, "x", 2)
    fars = [shift(grad_own, "x", 1), opposite, shift(grad_own, "x", 3)]
    for block in fars:
        grads += [block, shift(block, "core", 1)]

    mine, theirs = grad_normed(table, grad_own, grad_other, near + more + far)
    left_own, right_own = near[:2], [near[4], near[6], near[7], far[2]]
    halves = grad_weight_part(unit_place, columns, grads, left_own, right_own)
    group = ("zlo", "y", "zhi")
    arrived = lax.all_to_all(halves[0], group, 0, 0, tiled=True)
    arrived, later = lax.optimization_barrier((arrived, halves[1]))
    arrived = jnp.sum(arrived.astype(F32), axis=0)
    cut = kv_weight.shape[0] // 2
    sums = arrived[cut:]
    grad_gain = gather_gain(sums[0] + sums[1] + sums[2]) / norm_gain
    rest = lax.all_to_all(later, group, 0, 0, tiled=True)
    grad_weight = rows([arrived[:cut], jnp.sum(rest.astype(F32), axis=0)])
    theirs = shift(theirs, "core", 1)
    grad_input = norm_back(core, mine, theirs, source, inv, gain)
    return attended[None], grad_queries[None], grad_input[None], grad_weight, grad_gain


def solution(mesh):
    fine = Mesh(mesh.devices.reshape(tuple(SIZES.values())), tuple(SIZES))
    tokens = P(BLK, SEQ, None)
    weight = P(BLK + SEQ, None)
    return jax.shard_map(
        step,
        mesh=fine,
        in_specs=(tokens, tokens, tokens, P(BLK, SEQ), weight, P()),
        out_specs=(tokens, tokens, tokens, weight, P()),
        check_vma=False,
    )
```
